256 devices in a mesh: ens: 2 (over y_hi), time: 32 (over z, x), chan: 4 (over y_lo, core).
Axes of the slice: x: 4, y: 4 (y_hi: 2, y_lo: 2; y = y_hi * 2 + y_lo), z: 8, core: 2. Of those that a mesh axis runs over, the one named last changes fastest.
Arguments:
- decay_rate: float32 [4, 32768, 1024], P('ens', 'time', 'chan'), parts along dimension 0, may hold values from 0.2 to 2
- drive_in: bfloat16 [4, 32768, 1024], P('ens', 'time', 'chan'), parts along dimension 0, may hold values from -6 to 6
- gate_in: bfloat16 [4, 32768, 1024], P('ens', 'time', 'chan'), parts along dimension 0, may hold values from -6 to 6
- norm_gain: float32 [2048], P(('ens', 'chan')), parts along dimension 0, may hold values from 0.25 to 1.75
Outputs:
- mixed_out: bfloat16 [4, 32768, 1024], P('ens', 'time', 'chan'), parts along dimension 0
The draws below stay inside these ranges and needn't reach their ends.
There are 2 independent parts, one for each index of `ens`. The reference program is written for one: setup_inputs(seed, part) draws one part's arguments, and reference() takes and returns one part's arrays. A program takes and returns all parts, laid end to end along the dimension named above; each array names one. Nothing has to cross between parts.
All inputs are finite; a program needn't handle non-finite values.
Results may differ from the reference program's by a relative error of at most 0.001.
Values sent between devices are 32-bit elements.
A program may use at most 64 MiB of HBM per device.

```python
import jax
import jax.numpy as jnp
from jax import lax

BATCH = 2
CHANNELS = 1024
LENGTH = 32768


def steps_of(stream_key, shape, pieces, least, high):
    level = 1.0
    for dim, parts in pieces:
        steps = jax.random.uniform(jax.random.fold_in(jax.random.fold_in(stream_key, 6), dim), (parts,), jnp.float32, least / len(pieces), high / len(pieces))
        level = level * jnp.repeat(jnp.exp(steps), shape[dim] // parts).reshape((-1,) + (1,) * (len(shape) - 1 - dim))
    return level


def scatter_about(key, dims, width, limit, shards=(), held_as=jnp.bfloat16):
    entries = width * jax.random.normal(key, dims, jnp.float32)
    if shards:
        entries = entries * steps_of(key, dims, shards, -0.22, 0.18)
    return jnp.clip(entries, -limit, limit).astype(held_as)


def setup_inputs(seed: int = 0, part: int = 0) -> dict:
    seeds = jax.random.split(jax.random.key(seed), 5)
    part_keys = jax.random.split(jax.random.fold_in(seeds[4], part), 5)
    return {
        "decay_rate": jnp.clip(0.2 + 1.8 * jax.random.uniform(part_keys[0], (BATCH, LENGTH, CHANNELS), jnp.float32) ** steps_of(part_keys[0], (BATCH, LENGTH, CHANNELS), ((1, 32), (2, 4)), -0.2, 0.2), 0.2, 2.0),
        "drive_in": scatter_about(part_keys[1], (BATCH, LENGTH, CHANNELS), 1.0, 6.0, ((1, 32), (2, 4))),
        "gate_in": scatter_about(part_keys[2], (BATCH, LENGTH, CHANNELS), 1.0, 6.0, ((1, 32), (2, 4))),
        "norm_gain": jnp.clip(1.0 + 0.15 * jax.random.normal(part_keys[3], (CHANNELS,), jnp.float32), 0.25, 1.75),
    }


def join_pair(earlier, later):
    return (earlier[0] * later[0], later[0] * earlier[1] + later[1])

def reference(decay_rate, drive_in, gate_in, norm_gain):
    keep = jnp.exp(-decay_rate / LENGTH)
    push = drive_in.astype(jnp.float32) * LENGTH ** (-0.5)
    forward = lax.associative_scan(join_pair, (keep, push), axis=1)[1]
    backward = lax.associative_scan(join_pair, (keep, push), axis=1, reverse=True)[1]
    states = forward + backward
    gated = states * jax.nn.silu(gate_in.astype(jnp.float32))
    power = lax.optimization_barrier(jnp.mean(gated * gated, axis=-1, keepdims=True))
    mixed_out = (gated * lax.rsqrt(power + 1e-06) * norm_gain).astype(jnp.bfloat16)
    return mixed_out
```

```python
import functools

import jax
import jax.numpy as jnp
from jax import lax
from jax.experimental import pallas as pl
from jax.experimental.pallas import tpu as pltpu
from jax.sharding import PartitionSpec as P

F32, BF16 = jnp.float32, jnp.bfloat16
BLOCK = 256
CHUNK = 32
LANES = 128


def dot(a, b):
    return lax.dot_general(a, b, (((1,), (0,)), ((), ())), preferred_element_type=F32)


def peers_by_distance(count, width):
    rows = count // width
    away = lambda s, n: min(s, n - s)
    shifts = [(r, c) for r in range(rows) for c in range(width) if r or c]
    return sorted(shifts, key=lambda s: -(away(s[0], rows) + away(s[1], width)))


def kernel(
    times, chans, width,
    decay_hbm, drive_hbm, gate_hbm, gain_ref, out_hbm,
    decay, drive, gate, cum, up, down, base, into, back, result,
    note, notes, entry, power, powers,
    in_sem, out_sem, time_send, time_recv, chan_send, chan_recv,
):
    batch, length, channels = decay.shape
    blocks = length // BLOCK
    each = [(b, k) for b in range(batch) for k in range(blocks)]
    rows_of = lambda k: pl.ds(k * BLOCK, BLOCK)
    per_length = 1.0 / (length * times)
    t_me, c_me = lax.axis_index("time"), lax.axis_index("chan")
    row, column = t_me // width, t_me % width
    tall = times // width
    t_peers = [
        ((row + r) % tall) * width + (column + c) % width
        for r, c in peers_by_distance(times, width)
    ]
    c_peers = [(c_me + s) % chans for s in range(1, chans)]

    barrier = pltpu.get_barrier_semaphore()
    for peer in t_peers:
        pl.semaphore_signal(barrier, 1, device_id={"time": peer})
    for peer in c_peers:
        pl.semaphore_signal(barrier, 1, device_id={"chan": peer})

    def fetch(which, b, k):
        source, target = ((decay_hbm, decay), (drive_hbm, drive), (gate_hbm, gate))[which]
        return pltpu.make_async_copy(
            source.at[b, rows_of(k), :], target.at[b, rows_of(k), :], in_sem.at[which, b * blocks + k]
        )

    for b, k in each:
        fetch(0, b, k).start()
        fetch(1, b, k).start()
    for b, k in each:
        fetch(2, b, k).start()

    iota = lambda d: lax.broadcasted_iota(jnp.int32, (BLOCK, BLOCK), d)
    lower = jnp.where(iota(0) >= iota(1), 1.0, 0.0).astype(BF16)
    upper = jnp.where(iota(0) <= iota(1), 1.0, 0.0).astype(BF16)

    shrink, gain_up, gain_down = {}, {}, {}
    for b, k in each:
        fetch(0, b, k).wait()
        whole = decay[b, rows_of(k), :]
        high = whole.astype(BF16)
        low = (whole - high.astype(F32)).astype(BF16)
        cum[b, rows_of(k), :] = dot(lower, high) + dot(lower, low)
        fetch(1, b, k).wait()
        plain = rising = falling = jnp.zeros((8, channels), F32)
        for r in range(0, BLOCK, CHUNK):
            at = pl.ds(k * BLOCK + r, CHUNK)
            logs = cum[b, at, :] * per_length
            step = decay[b, at, :] * per_length
            push = drive[b, at, :].astype(F32)
            u = push * (jnp.exp(logs) - 1.0)
            v = push * (jnp.exp(step - logs) - 1.0)
            up[b, at, :] = u.astype(BF16)
            down[b, at, :] = v.astype(BF16)
            fold = lambda a: jnp.sum(a.reshape(CHUNK // 8, 8, channels), axis=0)
            plain, rising, falling = plain + fold(push), rising + fold(u), falling + fold(v)
        total = lambda a: jnp.sum(a, axis=0, keepdims=True)
        shrink[b, k] = jnp.exp(cum[b, pl.ds((k + 1) * BLOCK - 1, 1), :] * -per_length)
        gain_up[b, k] = total(plain + rising)
        gain_down[b, k] = total(plain + falling)

    for b in range(batch):
        kept = shrink[b, 0]
        ahead = shrink[b, 0] * gain_up[b, 0]
        for k in range(1, blocks):
            kept = kept * shrink[b, k]
            ahead = shrink[b, k] * (ahead + gain_up[b, k])
        behind = gain_down[b, blocks - 1]
        for k in reversed(range(blocks - 1)):
            behind = shrink[b, k] * behind + gain_down[b, k]
        for h in range(channels // LANES):
            lanes = slice(h * LANES, (h + 1) * LANES)
            r = b * (channels // LANES) + h
            for way, state in ((0, ahead), (1, behind)):
                note[way, r : r + 1, :] = kept[:, lanes]
                note[way, 4 + r : 5 + r, :] = state[:, lanes]

    pl.semaphore_wait(barrier, len(t_peers) + len(c_peers))

    def tell(peer):
        return pltpu.make_async_remote_copy(
            src_ref=note.at[jnp.where(peer > t_me, 0, 1)],
            dst_ref=notes.at[t_me],
            send_sem=time_send.at[peer],
            recv_sem=time_recv.at[t_me],
            device_id={"time": peer},
        )

    def told(peer):
        return pltpu.make_async_remote_copy(
            src_ref=note.at[0],
            dst_ref=notes.at[peer],
            send_sem=time_send.at[peer],
            recv_sem=time_recv.at[peer],
            device_id={"time": peer},
        )

    for peer in t_peers:
        tell(peer).start()
    notes[t_me] = note[0]

    for b, k in each:
        push = drive[b, rows_of(k), :]
        base[b, rows_of(k), :] = dot(lower, push) + dot(lower, up[b, rows_of(k), :])
        into[b, rows_of(k), :] = dot(upper, push) + dot(upper, down[b, rows_of(k), :])
        fetch(2, b, k).wait()
        for r in range(0, BLOCK, CHUNK):
            at = pl.ds(k * BLOCK + r, CHUNK)
            logs = cum[b, at, :] * per_length
            step = decay[b, at, :] * per_length
            g = gate[b, at, :].astype(F32)
            g = g * ((length * times) ** -0.5) / (1.0 + jnp.exp(-g))
            p, q = g * jnp.exp(-logs), g * jnp.exp(logs - step)
            base[b, at, :] = p * base[b, at, :] + q * into[b, at, :]
            into[b, at, :] = p
            back[b, at, :] = q

    for peer in t_peers:
        told(peer).wait_recv()
    ahead = behind = jnp.zeros((8, LANES), F32)
    for t in range(times):
        one = notes[t]
        ahead = jnp.where(t < t_me, ahead * pltpu.roll(one, 4, 0) + one, ahead)
        one = notes[times - 1 - t]
        behind = jnp.where(times - 1 - t > t_me, behind * pltpu.roll(one, 4, 0) + one, behind)
    entry[0] = ahead
    entry[1] = behind

    lane = lax.broadcasted_iota(jnp.int32, (CHUNK, LANES), 1)
    group = lax.broadcasted_iota(jnp.int32, (CHUNK, LANES), 0) // 8

    def share(b, peer):
        return pltpu.make_async_remote_copy(
            src_ref=power.at[b],
            dst_ref=powers.at[c_me, b],
            send_sem=chan_send.at[peer, b],
            recv_sem=chan_recv.at[c_me, b],
            device_id={"chan": peer},
        )

    def shared(b, peer):
        return pltpu.make_async_remote_copy(
            src_ref=power.at[b],
            dst_ref=powers.at[peer, b],
            send_sem=chan_send.at[peer, b],
            recv_sem=chan_recv.at[peer, b],
            device_id={"chan": peer},
        )

    gain = gain_ref[...]
    for b in range(batch):
        row_of = lambda way: jnp.concatenate(
            [entry[way, 4 + 2 * b + h : 5 + 2 * b + h, :] for h in range(channels // LANES)], axis=1
        )
        entering = {0: row_of(0)}
        for k in range(blocks - 1):
            entering[k + 1] = shrink[b, k] * (entering[k] + gain_up[b, k])
        leaving = {blocks - 1: shrink[b, blocks - 1] * row_of(1)}
        for k in reversed(range(blocks - 1)):
            leaving[k] = shrink[b, k] * (leaving[k + 1] + gain_down[b, k + 1])
        squares = jnp.zeros((8, LANES), F32)
        for k in range(blocks):
            for r in range(0, BLOCK, CHUNK):
                at = pl.ds(k * BLOCK + r, CHUNK)
                y = base[b, at, :] + into[b, at, :] * entering[k] + back[b, at, :] * leaving[k]
                base[b, at, :] = y * gain
                y = y * y
                y = y[:, :LANES] + y[:, LANES:]
                y = jnp.sum(y, axis=1, keepdims=True)
                y = jnp.where(lane == group + (k * BLOCK + r) // 8, y, 0.0)
                squares = squares + jnp.sum(y.reshape(CHUNK // 8, 8, LANES), axis=0)
        power[b] = squares
        for peer in c_peers:
            share(b, peer).start()

    ones = jnp.ones((2 * LANES, channels), BF16)
    lane = lax.broadcasted_iota(jnp.int32, (BLOCK, LANES), 1)
    group = lax.broadcasted_iota(jnp.int32, (BLOCK, LANES), 0) // 8
    for b in range(batch):
        squares = power[b]
        for peer in c_peers:
            shared(b, peer).wait_recv()
            squares = squares + powers[peer, b]
        scale = lax.rsqrt(squares * (1.0 / (channels * chans)) + 1e-06)
        high = scale.astype(BF16).astype(F32)
        tile = lambda a: jnp.concatenate([a] * (BLOCK // 8), axis=0)
        high, low = tile(high), tile(scale - high)
        for k in range(blocks):
            mine = lane == group + k * (BLOCK // 8)
            spread = [jnp.where(mine, a, 0.0).astype(BF16) for a in (high, low)]
            spread = dot(jnp.concatenate(spread, axis=1), ones)
            result[b, rows_of(k), :] = (base[b, rows_of(k), :] * spread).astype(BF16)
            pltpu.make_async_copy(
                result.at[b, rows_of(k), :], out_hbm.at[b, rows_of(k), :], out_sem.at[b * blocks + k]
            ).start()

    for peer in t_peers:
        told(peer).wait_send()
    for b in range(batch):
        for peer in c_peers:
            shared(b, peer).wait_send()
    for b, k in each:
        pltpu.make_async_copy(
            result.at[b, rows_of(k), :], out_hbm.at[b, rows_of(k), :], out_sem.at[b * blocks + k]
        ).wait()


def on_device(times, chans, decay_rate, drive_in, gate_in, norm_gain):
    shape = decay_rate.shape
    batch, length, channels = shape
    steps = batch * length // BLOCK
    width = 4 if times % 4 == 0 else 1
    big = lambda dtype: pltpu.VMEM(shape, dtype)
    tiles = lambda *lead: pltpu.VMEM((*lead, 8, LANES), F32)
    sems = lambda *dims: pltpu.SemaphoreType.DMA(dims)
    anywhere = pl.BlockSpec(memory_space=pl.ANY)
    return pl.pallas_call(
        functools.partial(kernel, times, chans, width),
        out_shape=jax.ShapeDtypeStruct(shape, BF16),
        in_specs=[anywhere, anywhere, anywhere, pl.BlockSpec(memory_space=pltpu.VMEM)],
        out_specs=anywhere,
        scratch_shapes=[
            big(F32), big(BF16), big(BF16),
            big(F32), big(BF16), big(BF16),
            big(F32), big(F32), big(F32), big(BF16),
            tiles(2), tiles(times), tiles(2), tiles(batch), tiles(chans, batch),
            sems(3, steps), sems(steps), sems(times), sems(times), sems(chans, batch), sems(chans, batch),
        ],
        compiler_params=pltpu.CompilerParams(
            collective_id=0, has_side_effects=True, vmem_limit_bytes=48 * 1024 * 1024
        ),
        name="two_way_scan",
    )(decay_rate, drive_in, gate_in, norm_gain.reshape(1, channels))


def solution(mesh):
    spec = P("ens", "time", "chan")
    return jax.shard_map(
        functools.partial(on_device, mesh.shape["time"], mesh.shape["chan"]),
        mesh=mesh,
        in_specs=(spec, spec, spec, P(("ens", "chan"))),
        out_specs=spec,
        check_vma=False,
    )
```

```python
import functools
import math

import jax
import jax.numpy as jnp
from jax import lax
from jax.experimental import pallas as pl
from jax.experimental.pallas import tpu as pltpu
from jax.sharding import PartitionSpec as P

F32, BF16 = jnp.float32, jnp.bfloat16
BLOCK = 256
CHUNK = 32
LANES = 128


def dot(a, b):
    return lax.dot_general(a, b, (((1,), (0,)), ((), ())), preferred_element_type=F32)


def peers_by_distance(count, width):
    rows = count // width
    away = lambda s, n: min(s, n - s)
    shifts = [(r, c) for r in range(rows) for c in range(width) if r or c]
    return sorted(shifts, key=lambda s: -(away(s[0], rows) + away(s[1], width)))


def kernel(
    times, chans, width,
    decay_hbm, drive_hbm, gate_hbm, gain_hbm, result,
    decay, drive, gate, gain_ref, cum, up, down, base, into, back,
    note, notes, entry, power, powers,
    in_sem, send_sem, time_recv, chan_recv,
):
    batch, length, channels = decay.shape
    blocks, halves = length // BLOCK, channels // LANES
    each = [(b, k) for b in range(batch) for k in range(blocks)]
    rows_of = lambda k: pl.ds(k * BLOCK, BLOCK)
    chunks_of = lambda k: [pl.ds(k * BLOCK + r, CHUNK) for r in range(0, BLOCK, CHUNK)]
    fold = lambda a: jnp.sum(a.reshape(CHUNK // 8, 8, a.shape[1]), axis=0)
    total = lambda a: jnp.sum(a, axis=0, keepdims=True)
    to_power = math.log2(math.e) / (length * times)

    with jax.named_scope("start"):
        fetches = {}
        for b in range(batch):
            fetches["decay", b] = pltpu.make_async_copy(decay_hbm.at[b], decay.at[b], in_sem.at[2 * b])
            fetches["drive", b] = pltpu.make_async_copy(drive_hbm.at[b], drive.at[b], in_sem.at[2 * b + 1])
        fetches["gate"] = pltpu.make_async_copy(gate_hbm, gate, in_sem.at[2 * batch])
        fetches["gain"] = pltpu.make_async_copy(gain_hbm, gain_ref, in_sem.at[2 * batch + 1])
        for fetch in fetches.values():
            fetch.start()

    t_me, c_me = lax.axis_index("time"), lax.axis_index("chan")
    with jax.named_scope("greet"):
        tall = times // width
        shift = lambda at, by, count: jnp.where(at + by >= count, at + by - count, at + by)
        rows = [shift(t_me // width, r, tall) * width for r in range(tall)]
        columns = [shift(t_me % width, c, width) for c in range(width)]
        t_peers = [rows[r] + columns[c] for r, c in peers_by_distance(times, width)]
        c_peers = [shift(c_me, s, chans) for s in range(1, chans)]
        barrier = pltpu.get_barrier_semaphore()
        for peer in t_peers:
            pl.semaphore_signal(barrier, 1, device_id={"time": peer})
        for peer in c_peers:
            pl.semaphore_signal(barrier, 1, device_id={"chan": peer})

    iota = lambda d: lax.broadcasted_iota(jnp.int32, (BLOCK, BLOCK), d)
    lower = jnp.where(iota(0) >= iota(1), 1.0, 0.0).astype(BF16)
    upper = jnp.where(iota(0) <= iota(1), 1.0, 0.0).astype(BF16)

    shrink, gain_up, gain_down = {}, {}, {}

    def add_up(b, k):
        rising = falling = jnp.zeros((8, channels), F32)
        for at in chunks_of(k):
            logs = cum[b, at, :]
            push = drive[b, at, :].astype(F32)
            u = push * (jnp.exp2(logs * to_power) - 1.0)
            v = push * (jnp.exp2((decay[b, at, :] - logs) * to_power) - 1.0)
            up[b, at, :] = u.astype(BF16)
            down[b, at, :] = v.astype(BF16)
            rising, falling = rising + fold(u + push), falling + fold(v + push)
        shrink[b, k] = jnp.exp2(cum[b, pl.ds((k + 1) * BLOCK - 1, 1), :] * -to_power)
        gain_up[b, k] = total(rising)
        gain_down[b, k] = total(falling)

    with jax.named_scope("sums"):
        for b in range(batch):
            fetches["decay", b].wait()
            fetches["drive", b].wait()
            for k in range(blocks + 1):
                if k < blocks:
                    whole = decay[b, rows_of(k), :]
                    high = whole.astype(BF16)
                    low = (whole - high.astype(F32)).astype(BF16)
                    cum[b, rows_of(k), :] = dot(lower, high) + dot(lower, low)
                if k > 0:
                    add_up(b, k - 1)

    with jax.named_scope("summary"):
        for b in range(batch):
            kept = shrink[b, 0]
            ahead = shrink[b, 0] * gain_up[b, 0]
            for k in range(1, blocks):
                kept = kept * shrink[b, k]
                ahead = shrink[b, k] * (ahead + gain_up[b, k])
            behind = gain_down[b, blocks - 1]
            for k in reversed(range(blocks - 1)):
                behind = shrink[b, k] * behind + gain_down[b, k]
            for h in range(halves):
                lanes = slice(h * LANES, (h + 1) * LANES)
                r = b * halves + h
                for way, state in ((0, ahead), (1, behind)):
                    note[way, r : r + 1, :] = kept[:, lanes]
                    note[way, 4 + r : 5 + r, :] = state[:, lanes]

    with jax.named_scope("meet"):
        pl.semaphore_wait(barrier, len(t_peers) + len(c_peers))

    with jax.named_scope("send"):
        for peer in t_peers:
            pltpu.make_async_remote_copy(
                src_ref=note.at[jnp.where(peer > t_me, 0, 1)],
                dst_ref=notes.at[t_me],
                send_sem=send_sem.at[0],
                recv_sem=time_recv,
                device_id={"time": peer},
            ).start()
        notes[t_me] = note[0]

    with jax.named_scope("inner"):
        fetches["gate"].wait()
        for n in range(len(each) + 1):
            if n < len(each):
                b, k = each[n]
                push = drive[b, rows_of(k), :]
                base[b, rows_of(k), :] = dot(lower, push) + dot(lower, up[b, rows_of(k), :])
                into[b, rows_of(k), :] = dot(upper, push) + dot(upper, down[b, rows_of(k), :])
            if n > 0:
                b, k = each[n - 1]
                for at in chunks_of(k):
                    logs = cum[b, at, :]
                    g = gate[b, at, :].astype(F32)
                    g = g * ((length * times) ** -0.5) / (1.0 + jnp.exp(-g))
                    p = g * jnp.exp2(logs * -to_power)
                    q = g * jnp.exp2((logs - decay[b, at, :]) * to_power)
                    base[b, at, :] = p * base[b, at, :] + q * into[b, at, :]
                    into[b, at, :] = p
                    back[b, at, :] = q

    def all_of(ref, count, sem):
        return pltpu.make_async_copy(ref.at[pl.ds(0, count)], ref.at[pl.ds(0, count)], sem)

    with jax.named_scope("receive"):
        all_of(notes, times - 1, time_recv).wait()

    with jax.named_scope("fold"):
        ahead = behind = jnp.zeros((8, LANES), F32)
        for t in range(times):
            one = notes[t]
            ahead = jnp.where(t < t_me, ahead * pltpu.roll(one, 4, 0) + one, ahead)
            one = notes[times - 1 - t]
            behind = jnp.where(times - 1 - t > t_me, behind * pltpu.roll(one, 4, 0) + one, behind)
        entry[0] = ahead
        entry[1] = behind

    lane = lax.broadcasted_iota(jnp.int32, (CHUNK, LANES), 1)
    group = lax.broadcasted_iota(jnp.int32, (CHUNK, LANES), 0) // 8
    with jax.named_scope("powers"):
        for b in range(batch):
            row_of = lambda way: jnp.concatenate(
                [entry[way, 4 + halves * b + h : 5 + halves * b + h, :] for h in range(halves)], axis=1
            )
            entering = {0: row_of(0)}
            for k in range(blocks - 1):
                entering[k + 1] = shrink[b, k] * (entering[k] + gain_up[b, k])
            leaving = {blocks - 1: shrink[b, blocks - 1] * row_of(1)}
            for k in reversed(range(blocks - 1)):
                leaving[k] = shrink[b, k] * (leaving[k + 1] + gain_down[b, k + 1])
            squares = jnp.zeros((8, LANES), F32)
            for k in range(blocks):
                for r, at in enumerate(chunks_of(k)):
                    y = base[b, at, :] + into[b, at, :] * entering[k] + back[b, at, :] * leaving[k]
                    base[b, at, :] = y
                    y = y * y
                    y = jnp.sum(y[:, :LANES] + y[:, LANES:], axis=1, keepdims=True)
                    squares = squares + fold(jnp.where(lane == group + (k * BLOCK + r * CHUNK) // 8, y, 0.0))
            power[b] = squares
            for peer in c_peers:
                pltpu.make_async_remote_copy(
                    src_ref=power.at[b],
                    dst_ref=powers.at[b, c_me],
                    send_sem=send_sem.at[1],
                    recv_sem=chan_recv.at[b],
                    device_id={"chan": peer},
                ).start()

    with jax.named_scope("gain"):
        fetches["gain"].wait()
        gain = gain_ref[...]
        for b, k in each:
            for at in chunks_of(k):
                base[b, at, :] = base[b, at, :] * gain

    ones = jnp.ones((2 * LANES, channels), BF16)
    lane = lax.broadcasted_iota(jnp.int32, (BLOCK, LANES), 1)
    group = lax.broadcasted_iota(jnp.int32, (BLOCK, LANES), 0) // 8
    with jax.named_scope("finish"):
        for b in range(batch):
            all_of(powers.at[b], chans - 1, chan_recv.at[b]).wait()
            powers[b, c_me] = power[b]
            squares = powers[b, 0]
            for c in range(1, chans):
                squares = squares + powers[b, c]
            scale = lax.rsqrt(squares * (1.0 / (channels * chans)) + 1e-06)
            high = scale.astype(BF16).astype(F32)
            tile = lambda a: jnp.concatenate([a] * (BLOCK // 8), axis=0)
            high, low = tile(high), tile(scale - high)
            for k in range(blocks):
                mine = lane == group + k * (BLOCK // 8)
                spread = [jnp.where(mine, a, 0.0).astype(BF16) for a in (high, low)]
                spread = dot(jnp.concatenate(spread, axis=1), ones)
                result[b, rows_of(k), :] = (base[b, rows_of(k), :] * spread).astype(BF16)

    with jax.named_scope("drain"):
        all_of(notes, times - 1, send_sem.at[0]).wait()
        all_of(notes, batch * (chans - 1), send_sem.at[1]).wait()


def on_device(times, chans, decay_rate, drive_in, gate_in, norm_gain):
    shape = decay_rate.shape
    batch, length, channels = shape
    arrays = decay_rate, drive_in, gate_in, norm_gain.reshape(1, channels)
    width = 4 if times % 4 == 0 else 1
    big = lambda dtype: pltpu.VMEM(shape, dtype)
    tiles = lambda *lead: pltpu.VMEM((*lead, 8, LANES), F32)
    sems = lambda *dims: pltpu.SemaphoreType.DMA(dims)
    anywhere = pl.BlockSpec(memory_space=pltpu.HBM)
    return pl.pallas_call(
        functools.partial(kernel, times, chans, width),
        out_shape=jax.ShapeDtypeStruct(shape, BF16),
        in_specs=[anywhere] * 4,
        out_specs=pl.BlockSpec(memory_space=pltpu.VMEM),
        scratch_shapes=[
            big(F32), big(BF16), big(BF16), pltpu.VMEM((1, channels), F32),
            big(F32), big(BF16), big(BF16), big(F32), big(F32), big(F32),
            tiles(2), tiles(times), tiles(2), tiles(batch), tiles(batch, chans),
            sems(2 * batch + 2), sems(2), sems(), sems(batch),
        ],
        compiler_params=pltpu.CompilerParams(
            collective_id=0, has_side_effects=True, vmem_limit_bytes=48 * 1024 * 1024
        ),
        name="two_way_scan",
    )(*[pltpu.with_memory_space_constraint(a, pltpu.HBM) for a in arrays])


def solution(mesh):
    spec = P("ens", "time", "chan")
    return jax.shard_map(
        functools.partial(on_device, mesh.shape["time"], mesh.shape["chan"]),
        mesh=mesh,
        in_specs=(spec, spec, spec, P(("ens", "chan"))),
        out_specs=spec,
        check_vma=False,
    )
```

```python
import functools
import math

import jax
import jax.numpy as jnp
from jax import lax
from jax.experimental import pallas as pl
from jax.experimental.pallas import tpu as pltpu
from jax.sharding import PartitionSpec as P

F32, BF16 = jnp.float32, jnp.bfloat16
BLOCK = 256
CHUNK = 32
LANES = 128


def dot(a, b):
    return lax.dot_general(a, b, (((1,), (0,)), ((), ())), preferred_element_type=F32)


def peers_by_distance(count, width):
    rows = count // width
    away = lambda s, n: min(s, n - s)
    shifts = [(r, c) for r in range(rows) for c in range(width) if r or c]
    return sorted(shifts, key=lambda s: -(away(s[0], rows) + away(s[1], width)))


class Both:
    def __init__(self, first, last):
        self.parts = first, last

    def of(self, at):
        first, last = self.parts
        return (last, at[1:]) if at[0] == first.shape[0] else (first, at)

    def __getitem__(self, at):
        ref, at = self.of(at)
        return ref[at]

    def __setitem__(self, at, value):
        ref, at = self.of(at)
        ref[at] = value


def spread_over(scale, blocks, channels):
    ones = jnp.ones((2 * LANES, channels), BF16)
    lane = lax.broadcasted_iota(jnp.int32, (BLOCK, LANES), 1)
    ahead = lane - lax.broadcasted_iota(jnp.int32, (BLOCK, LANES), 0) // 8
    high = scale.astype(BF16).astype(F32)
    tile = lambda a: jnp.concatenate([a] * (BLOCK // 8), axis=0)
    parts = tile(high), tile(scale - high)

    def block(k):
        mine = ahead == k * (BLOCK // 8)
        return dot(jnp.concatenate([jnp.where(mine, a, 0.0).astype(BF16) for a in parts], axis=1), ones)

    return [functools.partial(block, k) for k in range(blocks)]


def finish(done, last, scale, out_hbm, result, sem):
    before, length, channels = done.shape
    copies = [pltpu.make_async_copy(done, out_hbm.at[pl.ds(0, before)], sem.at[0])]
    copies[0].start()
    for k, spread in enumerate(spread_over(scale[...], length // BLOCK, channels)):
        at = pl.ds(k * BLOCK, BLOCK)
        result[at, :] = (last[at, :] * spread()).astype(BF16)
        copies.append(pltpu.make_async_copy(result.at[at, :], out_hbm.at[before, at, :], sem.at[k + 1]))
        copies[-1].start()
    for copy in copies:
        copy.wait()


def kernel(
    times, chans, width,
    decay_hbm, drive_hbm, gate_hbm, gain_hbm, done, last, last_scale,
    decay, drive, gate, gain_ref, cum, up, down, first, into, back,
    note, notes, entry, power, powers,
    in_sem, send_sem, time_recv, chan_recv,
):
    batch, length, channels = decay.shape
    blocks, halves = length // BLOCK, channels // LANES
    each = [(b, k) for b in range(batch) for k in range(blocks)]
    rows_of = lambda k: pl.ds(k * BLOCK, BLOCK)
    chunks_of = lambda k: [pl.ds(k * BLOCK + r, CHUNK) for r in range(0, BLOCK, CHUNK)]
    fold = lambda a: jnp.sum(a.reshape(CHUNK // 8, 8, a.shape[1]), axis=0)
    total = lambda a: jnp.sum(a, axis=0, keepdims=True)
    base = Both(first, last)
    to_power = math.log2(math.e) / (length * times)

    with jax.named_scope("start"):
        fetches = {}
        for b in range(batch):
            fetches["decay", b] = pltpu.make_async_copy(decay_hbm.at[b], decay.at[b], in_sem.at[2 * b])
            fetches["drive", b] = pltpu.make_async_copy(drive_hbm.at[b], drive.at[b], in_sem.at[2 * b + 1])
        fetches["gate"] = pltpu.make_async_copy(gate_hbm, gate, in_sem.at[2 * batch])
        fetches["gain"] = pltpu.make_async_copy(gain_hbm, gain_ref, in_sem.at[2 * batch + 1])
        for fetch in fetches.values():
            fetch.start()

    t_me, c_me = lax.axis_index("time"), lax.axis_index("chan")
    with jax.named_scope("greet"):
        tall = times // width
        shift = lambda at, by, count: jnp.where(at + by >= count, at + by - count, at + by)
        rows = [shift(t_me // width, r, tall) * width for r in range(tall)]
        columns = [shift(t_me % width, c, width) for c in range(width)]
        t_peers = [rows[r] + columns[c] for r, c in peers_by_distance(times, width)]
        c_peers = [shift(c_me, s, chans) for s in range(1, chans)]
        barrier = pltpu.get_barrier_semaphore()
        for peer in t_peers:
            pl.semaphore_signal(barrier, 1, device_id={"time": peer})
        for peer in c_peers:
            pl.semaphore_signal(barrier, 1, device_id={"chan": peer})

    iota = lambda d: lax.broadcasted_iota(jnp.int32, (BLOCK, BLOCK), d)
    lower = jnp.where(iota(0) >= iota(1), 1.0, 0.0).astype(BF16)
    upper = jnp.where(iota(0) <= iota(1), 1.0, 0.0).astype(BF16)

    shrink, gain_up, gain_down = {}, {}, {}

    def add_up(b, k):
        rising = falling = jnp.zeros((8, channels), F32)
        for at in chunks_of(k):
            logs = cum[b, at, :]
            push = drive[b, at, :].astype(F32)
            u = push * (jnp.exp2(logs * to_power) - 1.0)
            v = push * (jnp.exp2((decay[b, at, :] - logs) * to_power) - 1.0)
            up[b, at, :] = u.astype(BF16)
            down[b, at, :] = v.astype(BF16)
            rising, falling = rising + fold(u + push), falling + fold(v + push)
        shrink[b, k] = jnp.exp2(cum[b, pl.ds((k + 1) * BLOCK - 1, 1), :] * -to_power)
        gain_up[b, k] = total(rising)
        gain_down[b, k] = total(falling)

    with jax.named_scope("sums"):
        for b in range(batch):
            fetches["decay", b].wait()
            fetches["drive", b].wait()
            for k in range(blocks + 1):
                if k < blocks:
                    whole = decay[b, rows_of(k), :]
                    high = whole.astype(BF16)
                    low = (whole - high.astype(F32)).astype(BF16)
                    cum[b, rows_of(k), :] = dot(lower, high) + dot(lower, low)
                if k > 0:
                    add_up(b, k - 1)

    with jax.named_scope("summary"):
        for b in range(batch):
            kept = shrink[b, 0]
            ahead = shrink[b, 0] * gain_up[b, 0]
            for k in range(1, blocks):
                kept = kept * shrink[b, k]
                ahead = shrink[b, k] * (ahead + gain_up[b, k])
            behind = gain_down[b, blocks - 1]
            for k in reversed(range(blocks - 1)):
                behind = shrink[b, k] * behind + gain_down[b, k]
            for h in range(halves):
                lanes = slice(h * LANES, (h + 1) * LANES)
                r = b * halves + h
                for way, state in ((0, ahead), (1, behind)):
                    note[way, r : r + 1, :] = kept[:, lanes]
                    note[way, 4 + r : 5 + r, :] = state[:, lanes]

    with jax.named_scope("meet"):
        pl.semaphore_wait(barrier, len(t_peers) + len(c_peers))

    with jax.named_scope("send"):
        for peer in t_peers:
            pltpu.make_async_remote_copy(
                src_ref=note.at[jnp.where(peer > t_me, 0, 1)],
                dst_ref=notes.at[t_me],
                send_sem=send_sem.at[0],
                recv_sem=time_recv,
                device_id={"time": peer},
            ).start()
        notes[t_me] = note[0]

    with jax.named_scope("inner"):
        fetches["gate"].wait()
        for n in range(len(each) + 1):
            if n < len(each):
                b, k = each[n]
                push = drive[b, rows_of(k), :]
                base[b, rows_of(k), :] = dot(lower, push) + dot(lower, up[b, rows_of(k), :])
                into[b, rows_of(k), :] = dot(upper, push) + dot(upper, down[b, rows_of(k), :])
            if n > 0:
                b, k = each[n - 1]
                for at in chunks_of(k):
                    logs = cum[b, at, :]
                    g = gate[b, at, :].astype(F32)
                    g = g * ((length * times) ** -0.5) / (1.0 + jnp.exp(-g))
                    p = g * jnp.exp2(logs * -to_power)
                    q = g * jnp.exp2((logs - decay[b, at, :]) * to_power)
                    base[b, at, :] = p * base[b, at, :] + q * into[b, at, :]
                    into[b, at, :] = p
                    back[b, at, :] = q

    def all_of(ref, count, sem):
        return pltpu.make_async_copy(ref.at[pl.ds(0, count)], ref.at[pl.ds(0, count)], sem)

    with jax.named_scope("receive"):
        all_of(notes, times - 1, time_recv).wait()

    with jax.named_scope("fold"):
        ahead = behind = jnp.zeros((8, LANES), F32)
        for t in range(times):
            one = notes[t]
            ahead = jnp.where(t < t_me, ahead * pltpu.roll(one, 4, 0) + one, ahead)
            one = notes[times - 1 - t]
            behind = jnp.where(times - 1 - t > t_me, behind * pltpu.roll(one, 4, 0) + one, behind)
        entry[0] = ahead
        entry[1] = behind

    lane = lax.broadcasted_iota(jnp.int32, (CHUNK, LANES), 1)
    ahead_of = lane - lax.broadcasted_iota(jnp.int32, (CHUNK, LANES), 0) // 8
    with jax.named_scope("powers"):
        for b in range(batch):
            row_of = lambda way: jnp.concatenate(
                [entry[way, 4 + halves * b + h : 5 + halves * b + h, :] for h in range(halves)], axis=1
            )
            entering = {0: row_of(0)}
            for k in range(blocks - 1):
                entering[k + 1] = shrink[b, k] * (entering[k] + gain_up[b, k])
            leaving = {blocks - 1: shrink[b, blocks - 1] * row_of(1)}
            for k in reversed(range(blocks - 1)):
                leaving[k] = shrink[b, k] * (leaving[k + 1] + gain_down[b, k + 1])
            squares = jnp.zeros((8, LANES), F32)
            for k in range(blocks):
                for r, at in enumerate(chunks_of(k)):
                    y = base[b, at, :] + into[b, at, :] * entering[k] + back[b, at, :] * leaving[k]
                    base[b, at, :] = y
                    y = y * y
                    y = jnp.sum(y[:, :LANES] + y[:, LANES:], axis=1, keepdims=True)
                    squares = squares + fold(jnp.where(ahead_of == (k * BLOCK + r * CHUNK) // 8, y, 0.0))
            power[b] = squares
            for peer in c_peers:
                pltpu.make_async_remote_copy(
                    src_ref=power.at[b],
                    dst_ref=powers.at[b, c_me],
                    send_sem=send_sem.at[1],
                    recv_sem=chan_recv.at[b],
                    device_id={"chan": peer},
                ).start()

    with jax.named_scope("gain"):
        fetches["gain"].wait()
        gain = gain_ref[...]
        for b, k in each:
            for at in chunks_of(k):
                base[b, at, :] = base[b, at, :] * gain

    with jax.named_scope("finish"):
        for b in range(batch):
            all_of(powers.at[b], chans - 1, chan_recv.at[b]).wait()
            powers[b, c_me] = power[b]
            squares = powers[b, 0]
            for c in range(1, chans):
                squares = squares + powers[b, c]
            scale = lax.rsqrt(squares * (1.0 / (channels * chans)) + 1e-06)
            if b < batch - 1:
                for k, spread in enumerate(spread_over(scale, blocks, channels)):
                    done[b, rows_of(k), :] = (base[b, rows_of(k), :] * spread()).astype(BF16)
            else:
                last_scale[...] = scale

    with jax.named_scope("drain"):
        all_of(notes, times - 1, send_sem.at[0]).wait()
        all_of(notes, batch * (chans - 1), send_sem.at[1]).wait()


def on_device(times, chans, decay_rate, drive_in, gate_in, norm_gain):
    shape = decay_rate.shape
    batch, length, channels = shape
    arrays = decay_rate, drive_in, gate_in, norm_gain.reshape(1, channels)
    width = 4 if times % 4 == 0 else 1
    big = lambda dtype: pltpu.VMEM(shape, dtype)
    tiles = lambda *lead: pltpu.VMEM((*lead, 8, LANES), F32)
    sems = lambda *dims: pltpu.SemaphoreType.DMA(dims)
    anywhere = pl.BlockSpec(memory_space=pltpu.HBM)
    vmem = pl.BlockSpec(memory_space=pltpu.VMEM)
    done, last, scale = pl.pallas_call(
        functools.partial(kernel, times, chans, width),
        out_shape=(
            jax.ShapeDtypeStruct((batch - 1, length, channels), BF16),
            jax.ShapeDtypeStruct((length, channels), F32),
            jax.ShapeDtypeStruct((8, LANES), F32),
        ),
        in_specs=[anywhere] * 4,
        out_specs=(vmem, vmem, vmem),
        scratch_shapes=[
            big(F32), big(BF16), big(BF16), pltpu.VMEM((1, channels), F32),
            big(F32), big(BF16), big(BF16), pltpu.VMEM((batch - 1, length, channels), F32), big(F32), big(F32),
            tiles(2), tiles(times), tiles(2), tiles(batch), tiles(batch, chans),
            sems(2 * batch + 2), sems(2), sems(), sems(batch),
        ],
        compiler_params=pltpu.CompilerParams(
            collective_id=0, has_side_effects=True, vmem_limit_bytes=48 * 1024 * 1024
        ),
        name="two_way_scan",
    )(*[pltpu.with_memory_space_constraint(a, pltpu.HBM) for a in arrays])
    return pl.pallas_call(
        finish,
        out_shape=jax.ShapeDtypeStruct(shape, BF16),
        in_specs=[vmem, vmem, vmem],
        out_specs=anywhere,
        scratch_shapes=[pltpu.VMEM((length, channels), BF16), sems(length // BLOCK + 1)],
        compiler_params=pltpu.CompilerParams(vmem_limit_bytes=8 * 1024 * 1024),
        name="finish",
    )(done, last, scale)


def solution(mesh):
    spec = P("ens", "time", "chan")
    return jax.shard_map(
        functools.partial(on_device, mesh.shape["time"], mesh.shape["chan"]),
        mesh=mesh,
        in_specs=(spec, spec, spec, P(("ens", "chan"))),
        out_specs=spec,
        check_vma=False,
    )
```

```python
import functools
import math

import jax
import jax.numpy as jnp
from jax import lax
from jax.experimental import pallas as pl
from jax.experimental.pallas import tpu as pltpu
from jax.sharding import PartitionSpec as P

F32, BF16 = jnp.float32, jnp.bfloat16
BLOCK = 256
CHUNK = 32
LANES = 128


def dot(a, b):
    return lax.dot_general(a, b, (((1,), (0,)), ((), ())), preferred_element_type=F32)


def peers_by_distance(count, width):
    rows = count // width
    away = lambda s, n: min(s, n - s)
    shifts = [(r, c) for r in range(rows) for c in range(width) if r or c]
    return sorted(shifts, key=lambda s: -(away(s[0], rows) + away(s[1], width)))


class Both:
    def __init__(self, first, last):
        self.parts = first, last

    def of(self, at):
        first, last = self.parts
        return (last, at[1:]) if at[0] == first.shape[0] else (first, at)

    def __getitem__(self, at):
        ref, at = self.of(at)
        return ref[at]

    def __setitem__(self, at, value):
        ref, at = self.of(at)
        ref[at] = value


def spread_over(scale, blocks, channels):
    ones = jnp.ones((2 * LANES, channels), BF16)
    lane = lax.broadcasted_iota(jnp.int32, (BLOCK, LANES), 1)
    ahead = lane - lax.broadcasted_iota(jnp.int32, (BLOCK, LANES), 0) // 8
    high = scale.astype(BF16).astype(F32)
    tile = lambda a: jnp.concatenate([a] * (BLOCK // 8), axis=0)
    parts = tile(high), tile(scale - high)

    def block(k):
        mine = ahead == k * (BLOCK // 8)
        return dot(jnp.concatenate([jnp.where(mine, a, 0.0).astype(BF16) for a in parts], axis=1), ones)

    return [functools.partial(block, k) for k in range(blocks)]


def finish(done, last, scale, out_hbm, result, sem):
    before, length, channels = done.shape
    copies = [pltpu.make_async_copy(done, out_hbm.at[pl.ds(0, before)], sem.at[0])]
    copies[0].start()
    for k, spread in enumerate(spread_over(scale[...], length // BLOCK, channels)):
        at = pl.ds(k * BLOCK, BLOCK)
        result[at, :] = (last[at, :] * spread()).astype(BF16)
        copies.append(pltpu.make_async_copy(result.at[at, :], out_hbm.at[before, at, :], sem.at[k + 1]))
        copies[-1].start()
    for copy in copies:
        copy.wait()


def kernel(
    times, chans, width,
    decay_hbm, drive_hbm, gate_hbm, gain_hbm, done, last, last_scale,
    decay, drive, gate, gain_ref, cum, up, down, first, into, back,
    note, notes, entry, power, powers,
    in_sem, send_sem, time_recv, chan_recv,
):
    batch, length, channels = decay.shape
    blocks, halves = length // BLOCK, channels // LANES
    each = [(b, k) for b in range(batch) for k in range(blocks)]
    rows_of = lambda k: pl.ds(k * BLOCK, BLOCK)
    chunks_of = lambda k: [pl.ds(k * BLOCK + r, CHUNK) for r in range(0, BLOCK, CHUNK)]
    fold = lambda a: jnp.sum(a.reshape(CHUNK // 8, 8, a.shape[1]), axis=0)
    total = lambda a: jnp.sum(a, axis=0, keepdims=True)
    base = Both(first, last)
    to_power = math.log2(math.e) / (length * times)

    with jax.named_scope("start"):
        fetches = {}
        for b in range(batch):
            fetches["decay", b] = pltpu.make_async_copy(decay_hbm.at[b], decay.at[b], in_sem.at[2 * b])
            fetches["drive", b] = pltpu.make_async_copy(drive_hbm.at[b], drive.at[b], in_sem.at[2 * b + 1])
        fetches["gate"] = pltpu.make_async_copy(gate_hbm, gate, in_sem.at[2 * batch])
        fetches["gain"] = pltpu.make_async_copy(gain_hbm, gain_ref, in_sem.at[2 * batch + 1])
        for fetch in fetches.values():
            fetch.start()

    t_me, c_me = lax.axis_index("time"), lax.axis_index("chan")
    with jax.named_scope("greet"):
        tall = times // width
        shift = lambda at, by, count: jnp.where(at + by >= count, at + by - count, at + by)
        rows = [shift(t_me // width, r, tall) * width for r in range(tall)]
        columns = [shift(t_me % width, c, width) for c in range(width)]
        t_peers = [rows[r] + columns[c] for r, c in peers_by_distance(times, width)]
        c_peers = [shift(c_me, s, chans) for s in range(1, chans)]
        barrier = pltpu.get_barrier_semaphore()
        for peer in t_peers:
            pl.semaphore_signal(barrier, 1, device_id={"time": peer})
        for peer in c_peers:
            pl.semaphore_signal(barrier, 1, device_id={"chan": peer})

    iota = lambda d: lax.broadcasted_iota(jnp.int32, (BLOCK, BLOCK), d)
    lower = jnp.where(iota(0) >= iota(1), 1.0, 0.0).astype(BF16)
    upper = jnp.where(iota(0) <= iota(1), 1.0, 0.0).astype(BF16)

    shrink, gain_up, gain_down = {}, {}, {}

    def add_up(b, k):
        rising = falling = jnp.zeros((8, channels), F32)
        for at in chunks_of(k):
            logs = cum[b, at, :]
            push = drive[b, at, :].astype(F32)
            u = push * (jnp.exp2(logs * to_power) - 1.0)
            v = push * (jnp.exp2((decay[b, at, :] - logs) * to_power) - 1.0)
            up[b, at, :] = u.astype(BF16)
            down[b, at, :] = v.astype(BF16)
            rising, falling = rising + fold(u + push), falling + fold(v + push)
        shrink[b, k] = jnp.exp2(cum[b, pl.ds((k + 1) * BLOCK - 1, 1), :] * -to_power)
        gain_up[b, k] = total(rising)
        gain_down[b, k] = total(falling)

    with jax.named_scope("sums"):
        for b in range(batch):
            fetches["decay", b].wait()
            fetches["drive", b].wait()
            for k in range(blocks + 1):
                if k < blocks:
                    whole = decay[b, rows_of(k), :]
                    high = whole.astype(BF16)
                    low = (whole - high.astype(F32)).astype(BF16)
                    cum[b, rows_of(k), :] = dot(lower, high) + dot(lower, low)
                if k > 0:
                    add_up(b, k - 1)

    with jax.named_scope("summary"):
        for b in range(batch):
            kept = shrink[b, 0]
            ahead = shrink[b, 0] * gain_up[b, 0]
            for k in range(1, blocks):
                kept = kept * shrink[b, k]
                ahead = shrink[b, k] * (ahead + gain_up[b, k])
            behind = gain_down[b, blocks - 1]
            for k in reversed(range(blocks - 1)):
                behind = shrink[b, k] * behind + gain_down[b, k]
            for h in range(halves):
                lanes = slice(h * LANES, (h + 1) * LANES)
                r = b * halves + h
                for way, state in ((0, ahead), (1, behind)):
                    note[way, r : r + 1, :] = kept[:, lanes]
                    note[way, 4 + r : 5 + r, :] = state[:, lanes]

    with jax.named_scope("meet"):
        pl.semaphore_wait(barrier, len(t_peers) + len(c_peers))

    with jax.named_scope("send"):
        instead = t_peers[0]
        ordered = [jnp.where(t_me == 0, instead, 0)]
        ordered += [jnp.where(peer == 0, instead, peer) for peer in t_peers[1:]]
        for peer in ordered:
            pltpu.make_async_remote_copy(
                src_ref=note.at[jnp.where(peer > t_me, 0, 1)],
                dst_ref=notes.at[t_me],
                send_sem=send_sem.at[0],
                recv_sem=time_recv,
                device_id={"time": peer},
            ).start()
        notes[t_me] = note[0]

    with jax.named_scope("inner"):
        fetches["gate"].wait()
        for n in range(len(each) + 1):
            if n < len(each):
                b, k = each[n]
                push = drive[b, rows_of(k), :]
                base[b, rows_of(k), :] = dot(lower, push) + dot(lower, up[b, rows_of(k), :])
                into[b, rows_of(k), :] = dot(upper, push) + dot(upper, down[b, rows_of(k), :])
            if n > 0:
                b, k = each[n - 1]
                for at in chunks_of(k):
                    logs = cum[b, at, :]
                    g = gate[b, at, :].astype(F32)
                    g = g * ((length * times) ** -0.5) / (1.0 + jnp.exp(-g))
                    p = g * jnp.exp2(logs * -to_power)
                    q = g * jnp.exp2((logs - decay[b, at, :]) * to_power)
                    base[b, at, :] = p * base[b, at, :] + q * into[b, at, :]
                    into[b, at, :] = p
                    back[b, at, :] = q

    def all_of(ref, count, sem):
        return pltpu.make_async_copy(ref.at[pl.ds(0, count)], ref.at[pl.ds(0, count)], sem)

    with jax.named_scope("receive"):
        all_of(notes, times - 1, time_recv).wait()

    with jax.named_scope("fold"):
        ahead = behind = jnp.zeros((8, LANES), F32)
        for t in range(times):
            one = notes[t]
            ahead = jnp.where(t < t_me, ahead * pltpu.roll(one, 4, 0) + one, ahead)
            one = notes[times - 1 - t]
            behind = jnp.where(times - 1 - t > t_me, behind * pltpu.roll(one, 4, 0) + one, behind)
        entry[0] = ahead
        entry[1] = behind

    lane = lax.broadcasted_iota(jnp.int32, (CHUNK, LANES), 1)
    ahead_of = lane - lax.broadcasted_iota(jnp.int32, (CHUNK, LANES), 0) // 8
    with jax.named_scope("powers"):
        for b in range(batch):
            row_of = lambda way: jnp.concatenate(
                [entry[way, 4 + halves * b + h : 5 + halves * b + h, :] for h in range(halves)], axis=1
            )
            entering = {0: row_of(0)}
            for k in range(blocks - 1):
                entering[k + 1] = shrink[b, k] * (entering[k] + gain_up[b, k])
            leaving = {blocks - 1: shrink[b, blocks - 1] * row_of(1)}
            for k in reversed(range(blocks - 1)):
                leaving[k] = shrink[b, k] * (leaving[k + 1] + gain_down[b, k + 1])
            squares = jnp.zeros((8, LANES), F32)
            for k in range(blocks):
                for r, at in enumerate(chunks_of(k)):
                    y = base[b, at, :] + into[b, at, :] * entering[k] + back[b, at, :] * leaving[k]
                    base[b, at, :] = y
                    y = y * y
                    y = jnp.sum(y[:, :LANES] + y[:, LANES:], axis=1, keepdims=True)
                    squares = squares + fold(jnp.where(ahead_of == (k * BLOCK + r * CHUNK) // 8, y, 0.0))
            power[b] = squares
            for peer in c_peers:
                pltpu.make_async_remote_copy(
                    src_ref=power.at[b],
                    dst_ref=powers.at[b, c_me],
                    send_sem=send_sem.at[1],
                    recv_sem=chan_recv.at[b],
                    device_id={"chan": peer},
                ).start()

    with jax.named_scope("gain"):
        fetches["gain"].wait()
        gain = gain_ref[...]
        for b, k in each:
            for at in chunks_of(k):
                base[b, at, :] = base[b, at, :] * gain

    with jax.named_scope("finish"):
        for b in range(batch):
            all_of(powers.at[b], chans - 1, chan_recv.at[b]).wait()
            powers[b, c_me] = power[b]
            squares = powers[b, 0]
            for c in range(1, chans):
                squares = squares + powers[b, c]
            scale = lax.rsqrt(squares * (1.0 / (channels * chans)) + 1e-06)
            if b < batch - 1:
                for k, spread in enumerate(spread_over(scale, blocks, channels)):
                    done[b, rows_of(k), :] = (base[b, rows_of(k), :] * spread()).astype(BF16)
            else:
                last_scale[...] = scale

    with jax.named_scope("drain"):
        all_of(notes, times - 1, send_sem.at[0]).wait()
        all_of(notes, batch * (chans - 1), send_sem.at[1]).wait()


def on_device(times, chans, decay_rate, drive_in, gate_in, norm_gain):
    shape = decay_rate.shape
    batch, length, channels = shape
    arrays = decay_rate, drive_in, gate_in, norm_gain.reshape(1, channels)
    width = 4 if times % 4 == 0 else 1
    big = lambda dtype: pltpu.VMEM(shape, dtype)
    tiles = lambda *lead: pltpu.VMEM((*lead, 8, LANES), F32)
    sems = lambda *dims: pltpu.SemaphoreType.DMA(dims)
    anywhere = pl.BlockSpec(memory_space=pltpu.HBM)
    vmem = pl.BlockSpec(memory_space=pltpu.VMEM)
    done, last, scale = pl.pallas_call(
        functools.partial(kernel, times, chans, width),
        out_shape=(
            jax.ShapeDtypeStruct((batch - 1, length, channels), BF16),
            jax.ShapeDtypeStruct((length, channels), F32),
            jax.ShapeDtypeStruct((8, LANES), F32),
        ),
        in_specs=[anywhere] * 4,
        out_specs=(vmem, vmem, vmem),
        scratch_shapes=[
            big(F32), big(BF16), big(BF16), pltpu.VMEM((1, channels), F32),
            big(F32), big(BF16), big(BF16), pltpu.VMEM((batch - 1, length, channels), F32), big(F32), big(F32),
            tiles(2), tiles(times), tiles(2), tiles(batch), tiles(batch, chans),
            sems(2 * batch + 2), sems(2), sems(), sems(batch),
        ],
        compiler_params=pltpu.CompilerParams(
            collective_id=0, has_side_effects=True, vmem_limit_bytes=48 * 1024 * 1024
        ),
        name="two_way_scan",
    )(*[pltpu.with_memory_space_constraint(a, pltpu.HBM) for a in arrays])
    return pl.pallas_call(
        finish,
        out_shape=jax.ShapeDtypeStruct(shape, BF16),
        in_specs=[vmem, vmem, vmem],
        out_specs=anywhere,
        scratch_shapes=[pltpu.VMEM((length, channels), BF16), sems(length // BLOCK + 1)],
        compiler_params=pltpu.CompilerParams(vmem_limit_bytes=8 * 1024 * 1024),
        name="finish",
    )(done, last, scale)


def solution(mesh):
    spec = P("ens", "time", "chan")
    return jax.shard_map(
        functools.partial(on_device, mesh.shape["time"], mesh.shape["chan"]),
        mesh=mesh,
        in_specs=(spec, spec, spec, P(("ens", "chan"))),
        out_specs=spec,
        check_vma=False,
    )
```

```python
import functools
import math

import jax
import jax.numpy as jnp
from jax import lax
from jax.experimental import pallas as pl
from jax.experimental.pallas import tpu as pltpu
from jax.sharding import PartitionSpec as P

F32, BF16 = jnp.float32, jnp.bfloat16
BLOCK = 256
CHUNK = 32
LANES = 128


def dot(a, b):
    return lax.dot_general(a, b, (((1,), (0,)), ((), ())), preferred_element_type=F32)


def peers_by_distance(count, width):
    rows = count // width
    away = lambda s, n: min(s, n - s)
    shifts = [(r, c) for r in range(rows) for c in range(width) if r or c]
    return sorted(shifts, key=lambda s: -(away(s[0], rows) + away(s[1], width)))


class Both:
    def __init__(self, first, last):
        self.parts = first, last

    def of(self, at):
        first, last = self.parts
        return (last, at[1:]) if at[0] == first.shape[0] else (first, at)

    def __getitem__(self, at):
        ref, at = self.of(at)
        return ref[at]

    def __setitem__(self, at, value):
        ref, at = self.of(at)
        ref[at] = value


def spread_over(scale, blocks, channels):
    ones = jnp.ones((2 * LANES, channels), BF16)
    lane = lax.broadcasted_iota(jnp.int32, (BLOCK, LANES), 1)
    ahead = lane - lax.broadcasted_iota(jnp.int32, (BLOCK, LANES), 0) // 8
    high = scale.astype(BF16).astype(F32)
    tile = lambda a: jnp.concatenate([a] * (BLOCK // 8), axis=0)
    parts = tile(high), tile(scale - high)

    def block(k):
        mine = ahead == k * (BLOCK // 8)
        return dot(jnp.concatenate([jnp.where(mine, a, 0.0).astype(BF16) for a in parts], axis=1), ones)

    return [functools.partial(block, k) for k in range(blocks)]


def finish(done, last, scale, out_hbm, result, sem):
    before, length, channels = done.shape
    copies = [pltpu.make_async_copy(done, out_hbm.at[pl.ds(0, before)], sem.at[0])]
    copies[0].start()
    for k, spread in enumerate(spread_over(scale[...], length // BLOCK, channels)):
        at = pl.ds(k * BLOCK, BLOCK)
        result[at, :] = (last[at, :] * spread()).astype(BF16)
        copies.append(pltpu.make_async_copy(result.at[at, :], out_hbm.at[before, at, :], sem.at[k + 1]))
        copies[-1].start()
    for copy in copies:
        copy.wait()


def kernel(
    times, chans, width,
    decay_hbm, drive_hbm, gate_hbm, gain_hbm, done, last, last_scale,
    decay, drive, gate, gain_ref, cum, up, down, first, into, back,
    note, notes, entry, power, powers,
    in_sem, send_sem, time_recv, chan_recv,
):
    batch, length, channels = decay.shape
    blocks, halves = length // BLOCK, channels // LANES
    each = [(b, k) for b in range(batch) for k in range(blocks)]
    rows_of = lambda k: pl.ds(k * BLOCK, BLOCK)
    chunks_of = lambda k: [pl.ds(k * BLOCK + r, CHUNK) for r in range(0, BLOCK, CHUNK)]
    fold = lambda a: jnp.sum(a.reshape(CHUNK // 8, 8, a.shape[1]), axis=0)
    total = lambda a: jnp.sum(a, axis=0, keepdims=True)
    base = Both(first, last)
    to_power = math.log2(math.e) / (length * times)

    with jax.named_scope("start"):
        fetches = {}
        for b in range(batch):
            fetches["decay", b] = pltpu.make_async_copy(decay_hbm.at[b], decay.at[b], in_sem.at[2 * b])
            fetches["drive", b] = pltpu.make_async_copy(drive_hbm.at[b], drive.at[b], in_sem.at[2 * b + 1])
        fetches["gate"] = pltpu.make_async_copy(gate_hbm, gate, in_sem.at[2 * batch])
        fetches["gain"] = pltpu.make_async_copy(gain_hbm, gain_ref, in_sem.at[2 * batch + 1])
        for fetch in fetches.values():
            fetch.start()

    t_me, c_me = lax.axis_index("time"), lax.axis_index("chan")
    with jax.named_scope("greet"):
        tall = times // width
        shift = lambda at, by, count: jnp.where(at + by >= count, at + by - count, at + by)
        rows = [shift(t_me // width, r, tall) * width for r in range(tall)]
        columns = [shift(t_me % width, c, width) for c in range(width)]
        t_peers = [rows[r] + columns[c] for r, c in peers_by_distance(times, width)]
        c_peers = [shift(c_me, s, chans) for s in range(1, chans)]
        barrier = pltpu.get_barrier_semaphore()
        for peer in t_peers:
            pl.semaphore_signal(barrier, 1, device_id={"time": peer})
        for peer in c_peers:
            pl.semaphore_signal(barrier, 1, device_id={"chan": peer})

    iota = lambda d: lax.broadcasted_iota(jnp.int32, (BLOCK, BLOCK), d)
    lower = jnp.where(iota(0) >= iota(1), 1.0, 0.0).astype(BF16)
    upper = jnp.where(iota(0) <= iota(1), 1.0, 0.0).astype(BF16)

    shrink, gain_up, gain_down = {}, {}, {}

    def add_up(b, k):
        whole = plain = rising = falling = jnp.zeros((8, channels), F32)
        for at in chunks_of(k):
            logs, step = cum[b, at, :], decay[b, at, :]
            push = drive[b, at, :].astype(F32)
            u = push * (jnp.exp2(logs * to_power) - 1.0)
            v = push * (jnp.exp2((step - logs) * to_power) - 1.0)
            up[b, at, :] = u.astype(BF16)
            down[b, at, :] = v.astype(BF16)
            whole, plain = whole + fold(step), plain + fold(push)
            rising, falling = rising + fold(u), falling + fold(v)
        shrink[b, k] = jnp.exp2(total(whole) * -to_power)
        gain_up[b, k] = total(plain + rising)
        gain_down[b, k] = total(plain + falling)

    with jax.named_scope("sums"):
        for b in range(batch):
            fetches["decay", b].wait()
            fetches["drive", b].wait()
            for k in range(blocks + 1):
                if k < blocks:
                    cum[b, rows_of(k), :] = dot(lower, decay[b, rows_of(k), :].astype(BF16))
                if k > 0:
                    add_up(b, k - 1)

    with jax.named_scope("summary"):
        for b in range(batch):
            kept = shrink[b, 0]
            ahead = shrink[b, 0] * gain_up[b, 0]
            for k in range(1, blocks):
                kept = kept * shrink[b, k]
                ahead = shrink[b, k] * (ahead + gain_up[b, k])
            behind = gain_down[b, blocks - 1]
            for k in reversed(range(blocks - 1)):
                behind = shrink[b, k] * behind + gain_down[b, k]
            for h in range(halves):
                lanes = slice(h * LANES, (h + 1) * LANES)
                r = b * halves + h
                for way, state in ((0, ahead), (1, behind)):
                    note[way, r : r + 1, :] = kept[:, lanes]
                    note[way, 4 + r : 5 + r, :] = state[:, lanes]

    with jax.named_scope("meet"):
        pl.semaphore_wait(barrier, len(t_peers) + len(c_peers))

    with jax.named_scope("send"):
        instead = t_peers[0]
        ordered = [jnp.where(t_me == 0, instead, 0)]
        ordered += [jnp.where(peer == 0, instead, peer) for peer in t_peers[1:]]
        for peer in ordered:
            pltpu.make_async_remote_copy(
                src_ref=note.at[jnp.where(peer > t_me, 0, 1)],
                dst_ref=notes.at[t_me],
                send_sem=send_sem.at[0],
                recv_sem=time_recv,
                device_id={"time": peer},
            ).start()
        notes[t_me] = note[0]

    with jax.named_scope("inner"):
        fetches["gate"].wait()
        for n in range(len(each) + 1):
            if n < len(each):
                b, k = each[n]
                push = drive[b, rows_of(k), :]
                base[b, rows_of(k), :] = dot(lower, push) + dot(lower, up[b, rows_of(k), :])
                into[b, rows_of(k), :] = dot(upper, push) + dot(upper, down[b, rows_of(k), :])
            if n > 0:
                b, k = each[n - 1]
                for at in chunks_of(k):
                    logs = cum[b, at, :]
                    g = gate[b, at, :].astype(F32)
                    g = g * ((length * times) ** -0.5) / (1.0 + jnp.exp(-g))
                    p = g * jnp.exp2(logs * -to_power)
                    q = g * jnp.exp2((logs - decay[b, at, :]) * to_power)
                    base[b, at, :] = p * base[b, at, :] + q * into[b, at, :]
                    into[b, at, :] = p
                    back[b, at, :] = q

    def all_of(ref, count, sem):
        return pltpu.make_async_copy(ref.at[pl.ds(0, count)], ref.at[pl.ds(0, count)], sem)

    with jax.named_scope("receive"):
        all_of(notes, times - 1, time_recv).wait()

    with jax.named_scope("fold"):
        ahead = behind = jnp.zeros((8, LANES), F32)
        for t in range(times):
            one = notes[t]
            ahead = jnp.where(t < t_me, ahead * pltpu.roll(one, 4, 0) + one, ahead)
            one = notes[times - 1 - t]
            behind = jnp.where(times - 1 - t > t_me, behind * pltpu.roll(one, 4, 0) + one, behind)
        entry[0] = ahead
        entry[1] = behind

    lane = lax.broadcasted_iota(jnp.int32, (CHUNK, LANES), 1)
    ahead_of = lane - lax.broadcasted_iota(jnp.int32, (CHUNK, LANES), 0) // 8
    with jax.named_scope("powers"):
        for b in range(batch):
            row_of = lambda way: jnp.concatenate(
                [entry[way, 4 + halves * b + h : 5 + halves * b + h, :] for h in range(halves)], axis=1
            )
            entering = {0: row_of(0)}
            for k in range(blocks - 1):
                entering[k + 1] = shrink[b, k] * (entering[k] + gain_up[b, k])
            leaving = {blocks - 1: shrink[b, blocks - 1] * row_of(1)}
            for k in reversed(range(blocks - 1)):
                leaving[k] = shrink[b, k] * (leaving[k + 1] + gain_down[b, k + 1])
            squares = jnp.zeros((8, LANES), F32)
            for k in range(blocks):
                for r, at in enumerate(chunks_of(k)):
                    y = base[b, at, :] + into[b, at, :] * entering[k] + back[b, at, :] * leaving[k]
                    base[b, at, :] = y
                    y = y * y
                    y = jnp.sum(y[:, :LANES] + y[:, LANES:], axis=1, keepdims=True)
                    squares = squares + fold(jnp.where(ahead_of == (k * BLOCK + r * CHUNK) // 8, y, 0.0))
            power[b] = squares
            for peer in c_peers:
                pltpu.make_async_remote_copy(
                    src_ref=power.at[b],
                    dst_ref=powers.at[b, c_me],
                    send_sem=send_sem.at[1],
                    recv_sem=chan_recv.at[b],
                    device_id={"chan": peer},
                ).start()

    with jax.named_scope("gain"):
        fetches["gain"].wait()
        gain = gain_ref[...]
        for b, k in each:
            for at in chunks_of(k):
                base[b, at, :] = base[b, at, :] * gain

    with jax.named_scope("finish"):
        for b in range(batch):
            all_of(powers.at[b], chans - 1, chan_recv.at[b]).wait()
            powers[b, c_me] = power[b]
            squares = powers[b, 0]
            for c in range(1, chans):
                squares = squares + powers[b, c]
            scale = lax.rsqrt(squares * (1.0 / (channels * chans)) + 1e-06)
            if b < batch - 1:
                for k, spread in enumerate(spread_over(scale, blocks, channels)):
                    done[b, rows_of(k), :] = (base[b, rows_of(k), :] * spread()).astype(BF16)
            else:
                last_scale[...] = scale

    with jax.named_scope("drain"):
        all_of(notes, times - 1, send_sem.at[0]).wait()
        all_of(notes, batch * (chans - 1), send_sem.at[1]).wait()


def on_device(times, chans, decay_rate, drive_in, gate_in, norm_gain):
    shape = decay_rate.shape
    batch, length, channels = shape
    arrays = decay_rate, drive_in, gate_in, norm_gain.reshape(1, channels)
    width = 4 if times % 4 == 0 else 1
    big = lambda dtype: pltpu.VMEM(shape, dtype)
    tiles = lambda *lead: pltpu.VMEM((*lead, 8, LANES), F32)
    sems = lambda *dims: pltpu.SemaphoreType.DMA(dims)
    anywhere = pl.BlockSpec(memory_space=pltpu.HBM)
    vmem = pl.BlockSpec(memory_space=pltpu.VMEM)
    done, last, scale = pl.pallas_call(
        functools.partial(kernel, times, chans, width),
        out_shape=(
            jax.ShapeDtypeStruct((batch - 1, length, channels), BF16),
            jax.ShapeDtypeStruct((length, channels), F32),
            jax.ShapeDtypeStruct((8, LANES), F32),
        ),
        in_specs=[anywhere] * 4,
        out_specs=(vmem, vmem, vmem),
        scratch_shapes=[
            big(F32), big(BF16), big(BF16), pltpu.VMEM((1, channels), F32),
            big(F32), big(BF16), big(BF16), pltpu.VMEM((batch - 1, length, channels), F32), big(F32), big(F32),
            tiles(2), tiles(times), tiles(2), tiles(batch), tiles(batch, chans),
            sems(2 * batch + 2), sems(2), sems(), sems(batch),
        ],
        compiler_params=pltpu.CompilerParams(
            collective_id=0, has_side_effects=True, vmem_limit_bytes=48 * 1024 * 1024
        ),
        name="two_way_scan",
    )(*[pltpu.with_memory_space_constraint(a, pltpu.HBM) for a in arrays])
    return pl.pallas_call(
        finish,
        out_shape=jax.ShapeDtypeStruct(shape, BF16),
        in_specs=[vmem, vmem, vmem],
        out_specs=anywhere,
        scratch_shapes=[pltpu.VMEM((length, channels), BF16), sems(length // BLOCK + 1)],
        compiler_params=pltpu.CompilerParams(vmem_limit_bytes=8 * 1024 * 1024),
        name="finish",
    )(done, last, scale)


def solution(mesh):
    spec = P("ens", "time", "chan")
    return jax.shard_map(
        functools.partial(on_device, mesh.shape["time"], mesh.shape["chan"]),
        mesh=mesh,
        in_specs=(spec, spec, spec, P(("ens", "chan"))),
        out_specs=spec,
        check_vma=False,
    )
```

```python
import functools
import math

import jax
import jax.numpy as jnp
from jax import lax
from jax.experimental import pallas as pl
from jax.experimental.pallas import tpu as pltpu
from jax.sharding import PartitionSpec as P

F32, BF16 = jnp.float32, jnp.bfloat16
BLOCK = 256
CHUNK = 32
LANES = 128


def dot(a, b):
    return lax.dot_general(a, b, (((1,), (0,)), ((), ())), preferred_element_type=F32)


def peers_by_distance(count, width):
    rows = count // width
    away = lambda s, n: min(s, n - s)
    shifts = [(r, c) for r in range(rows) for c in range(width) if r or c]
    return sorted(shifts, key=lambda s: -(away(s[0], rows) + away(s[1], width)))


class Both:
    def __init__(self, first, last):
        self.parts = first, last

    def of(self, at):
        first, last = self.parts
        return (last, at[1:]) if at[0] == first.shape[0] else (first, at)

    def __getitem__(self, at):
        ref, at = self.of(at)
        return ref[at]

    def __setitem__(self, at, value):
        ref, at = self.of(at)
        ref[at] = value


def spreader(scale):
    iota = lambda d, shape: lax.broadcasted_iota(jnp.int32, shape, d)
    square = (2 * LANES, 2 * LANES)
    ones = jnp.where((iota(0, square) % 32 < 16) == (iota(1, square) < LANES), 1.0, 0.0).astype(BF16)
    lane = iota(1, (BLOCK // 2, LANES))
    ahead = lane % 16 + lane // 32 * 16 - iota(0, (BLOCK // 2, LANES)) // 8
    high = scale.astype(BF16).astype(F32)
    tile = lambda a: jnp.concatenate([a] * (BLOCK // 16), axis=0)
    parts = tile(high), tile(scale - high)

    def block(k):
        mine = ahead == k * 16
        both = dot(jnp.concatenate([jnp.where(mine, a, 0.0).astype(BF16) for a in parts], axis=1), ones)
        return [jnp.concatenate([half, half], axis=1) for half in (both[:, :LANES], both[:, LANES:])]

    return block


def finish(done, last, scale, out_hbm, result, sem):
    before, length, channels = done.shape
    copies = [pltpu.make_async_copy(done, out_hbm.at[pl.ds(0, before)], sem.at[0])]
    copies[0].start()
    spread_over = spreader(scale[...])
    for k in range(length // BLOCK):
        for h, spread in enumerate(spread_over(k)):
            at = pl.ds(k * BLOCK + h * BLOCK // 2, BLOCK // 2)
            result[at, :] = (last[at, :] * spread).astype(BF16)
        at = pl.ds(k * BLOCK, BLOCK)
        copies.append(pltpu.make_async_copy(result.at[at, :], out_hbm.at[before, at, :], sem.at[k + 1]))
        copies[-1].start()
    for copy in copies:
        copy.wait()


def kernel(
    times, chans, width,
    decay_hbm, drive_hbm, gate_hbm, gain_hbm, done, last, last_scale,
    decay, drive, gate, gain_ref, cum, up, down, first, into, back,
    note, notes, entry, power, powers,
    in_sem, send_sem, time_recv, chan_recv,
):
    batch, length, channels = decay.shape
    blocks, halves = length // BLOCK, channels // LANES
    each = [(b, k) for b in range(batch) for k in range(blocks)]
    rows_of = lambda k: pl.ds(k * BLOCK, BLOCK)
    chunks_of = lambda k: [pl.ds(k * BLOCK + r, CHUNK) for r in range(0, BLOCK, CHUNK)]
    fold = lambda a: jnp.sum(a.reshape(CHUNK // 8, 8, a.shape[1]), axis=0)
    total = lambda a: jnp.sum(a, axis=0, keepdims=True)
    base = Both(first, last)
    to_power = math.log2(math.e) / (length * times)

    with jax.named_scope("start"):
        fetches = {}
        for b in range(batch):
            fetches["decay", b] = pltpu.make_async_copy(decay_hbm.at[b], decay.at[b], in_sem.at[2 * b])
            fetches["drive", b] = pltpu.make_async_copy(drive_hbm.at[b], drive.at[b], in_sem.at[2 * b + 1])
        fetches["gate"] = pltpu.make_async_copy(gate_hbm, gate, in_sem.at[2 * batch])
        fetches["gain"] = pltpu.make_async_copy(gain_hbm, gain_ref, in_sem.at[2 * batch + 1])
        for fetch in fetches.values():
            fetch.start()

    t_me, c_me = lax.axis_index("time"), lax.axis_index("chan")
    with jax.named_scope("greet"):
        tall = times // width
        shift = lambda at, by, count: jnp.where(at + by >= count, at + by - count, at + by)
        rows = [shift(t_me // width, r, tall) * width for r in range(tall)]
        columns = [shift(t_me % width, c, width) for c in range(width)]
        t_peers = [rows[r] + columns[c] for r, c in peers_by_distance(times, width)]
        c_peers = [shift(c_me, s, chans) for s in range(1, chans)]
        barrier = pltpu.get_barrier_semaphore()
        for peer in t_peers:
            pl.semaphore_signal(barrier, 1, device_id={"time": peer})
        for peer in c_peers:
            pl.semaphore_signal(barrier, 1, device_id={"chan": peer})

    iota = lambda d: lax.broadcasted_iota(jnp.int32, (BLOCK, BLOCK), d)
    lower = jnp.where(iota(0) >= iota(1), 1.0, 0.0).astype(BF16)
    upper = jnp.where(iota(0) <= iota(1), 1.0, 0.0).astype(BF16)

    shrink, gain_up, gain_down = {}, {}, {}

    def add_up(b, k):
        whole = plain = rising = falling = jnp.zeros((8, channels), F32)
        for at in chunks_of(k):
            logs, step = cum[b, at, :], decay[b, at, :]
            push = drive[b, at, :].astype(F32)
            u = push * (jnp.exp2(logs * to_power) - 1.0)
            v = push * (jnp.exp2((step - logs) * to_power) - 1.0)
            up[b, at, :] = u.astype(BF16)
            down[b, at, :] = v.astype(BF16)
            whole, plain = whole + fold(step), plain + fold(push)
            rising, falling = rising + fold(u), falling + fold(v)
        shrink[b, k] = jnp.exp2(total(whole) * -to_power)
        gain_up[b, k] = total(plain + rising)
        gain_down[b, k] = total(plain + falling)

    with jax.named_scope("sums"):
        for b in range(batch):
            fetches["decay", b].wait()
            fetches["drive", b].wait()
            for k in range(blocks + 1):
                if k < blocks:
                    cum[b, rows_of(k), :] = dot(lower, decay[b, rows_of(k), :].astype(BF16))
                if k > 0:
                    add_up(b, k - 1)

    with jax.named_scope("summary"):
        for b in range(batch):
            kept = shrink[b, 0]
            ahead = shrink[b, 0] * gain_up[b, 0]
            for k in range(1, blocks):
                kept = kept * shrink[b, k]
                ahead = shrink[b, k] * (ahead + gain_up[b, k])
            behind = gain_down[b, blocks - 1]
            for k in reversed(range(blocks - 1)):
                behind = shrink[b, k] * behind + gain_down[b, k]
            for h in range(halves):
                lanes = slice(h * LANES, (h + 1) * LANES)
                r = b * halves + h
                for way, state in ((0, ahead), (1, behind)):
                    note[way, r : r + 1, :] = kept[:, lanes]
                    note[way, 4 + r : 5 + r, :] = state[:, lanes]

    with jax.named_scope("meet"):
        pl.semaphore_wait(barrier, len(t_peers) + len(c_peers))

    with jax.named_scope("send"):
        instead = t_peers[0]
        ordered = [jnp.where(t_me == 0, instead, 0)]
        ordered += [jnp.where(peer == 0, instead, peer) for peer in t_peers[1:]]
        for peer in ordered:
            pltpu.make_async_remote_copy(
                src_ref=note.at[jnp.where(peer > t_me, 0, 1)],
                dst_ref=notes.at[t_me],
                send_sem=send_sem.at[0],
                recv_sem=time_recv,
                device_id={"time": peer},
            ).start()
        notes[t_me] = note[0]

    with jax.named_scope("inner"):
        fetches["gate"].wait()
        for n in range(len(each) + 1):
            if n < len(each):
                b, k = each[n]
                push = drive[b, rows_of(k), :]
                base[b, rows_of(k), :] = dot(lower, push) + dot(lower, up[b, rows_of(k), :])
                into[b, rows_of(k), :] = dot(upper, push) + dot(upper, down[b, rows_of(k), :])
            if n > 0:
                b, k = each[n - 1]
                for at in chunks_of(k):
                    logs = cum[b, at, :]
                    g = gate[b, at, :].astype(F32)
                    g = g * ((length * times) ** -0.5) / (1.0 + jnp.exp(-g))
                    p = g * jnp.exp2(logs * -to_power)
                    q = g * jnp.exp2((logs - decay[b, at, :]) * to_power)
                    base[b, at, :] = p * base[b, at, :] + q * into[b, at, :]
                    into[b, at, :] = p
                    back[b, at, :] = q

    def all_of(ref, count, sem):
        return pltpu.make_async_copy(ref.at[pl.ds(0, count)], ref.at[pl.ds(0, count)], sem)

    with jax.named_scope("receive"):
        all_of(notes, times - 1, time_recv).wait()

    with jax.named_scope("fold"):
        ahead = behind = jnp.zeros((8, LANES), F32)
        for t in range(times):
            one = notes[t]
            ahead = jnp.where(t < t_me, ahead * pltpu.roll(one, 4, 0) + one, ahead)
            one = notes[times - 1 - t]
            behind = jnp.where(times - 1 - t > t_me, behind * pltpu.roll(one, 4, 0) + one, behind)
        entry[0] = ahead
        entry[1] = behind

    with jax.named_scope("powers"):
        for b in range(batch):
            row_of = lambda way: jnp.concatenate(
                [entry[way, 4 + halves * b + h : 5 + halves * b + h, :] for h in range(halves)], axis=1
            )
            entering = {0: row_of(0)}
            for k in range(blocks - 1):
                entering[k + 1] = shrink[b, k] * (entering[k] + gain_up[b, k])
            leaving = {blocks - 1: shrink[b, blocks - 1] * row_of(1)}
            for k in reversed(range(blocks - 1)):
                leaving[k] = shrink[b, k] * (leaving[k + 1] + gain_down[b, k + 1])
            for k in range(blocks):
                for r, at in enumerate(chunks_of(k)):
                    y = base[b, at, :] + into[b, at, :] * entering[k] + back[b, at, :] * leaving[k]
                    base[b, at, :] = y
                    y = y * y
                    y = jnp.sum(y[:, :LANES] + y[:, LANES:], axis=1, keepdims=True)
                    for g in range(CHUNK // 8):
                        q = (k * BLOCK + r * CHUNK) // 8 + g
                        power[b, :, q : q + 1] = y[8 * g : 8 * g + 8]
            for peer in c_peers:
                pltpu.make_async_remote_copy(
                    src_ref=power.at[b],
                    dst_ref=powers.at[b, c_me],
                    send_sem=send_sem.at[1],
                    recv_sem=chan_recv.at[b],
                    device_id={"chan": peer},
                ).start()

    with jax.named_scope("gain"):
        fetches["gain"].wait()
        gain = gain_ref[...]
        for b, k in each:
            for at in chunks_of(k):
                base[b, at, :] = base[b, at, :] * gain

    with jax.named_scope("finish"):
        for b in range(batch):
            all_of(powers.at[b], chans - 1, chan_recv.at[b]).wait()
            powers[b, c_me] = power[b]
            squares = powers[b, 0]
            for c in range(1, chans):
                squares = squares + powers[b, c]
            scale = lax.rsqrt(squares * (1.0 / (channels * chans)) + 1e-06)
            if b < batch - 1:
                spread_over = spreader(scale)
                for k in range(blocks):
                    for h, spread in enumerate(spread_over(k)):
                        at = pl.ds(k * BLOCK + h * BLOCK // 2, BLOCK // 2)
                        done[b, at, :] = (base[b, at, :] * spread).astype(BF16)
            else:
                last_scale[...] = scale

    with jax.named_scope("drain"):
        all_of(notes, times - 1, send_sem.at[0]).wait()
        all_of(notes, batch * (chans - 1), send_sem.at[1]).wait()


def on_device(times, chans, decay_rate, drive_in, gate_in, norm_gain):
    shape = decay_rate.shape
    batch, length, channels = shape
    arrays = decay_rate, drive_in, gate_in, norm_gain.reshape(1, channels)
    width = 4 if times % 4 == 0 else 1
    big = lambda dtype: pltpu.VMEM(shape, dtype)
    tiles = lambda *lead: pltpu.VMEM((*lead, 8, LANES), F32)
    sems = lambda *dims: pltpu.SemaphoreType.DMA(dims)
    anywhere = pl.BlockSpec(memory_space=pltpu.HBM)
    vmem = pl.BlockSpec(memory_space=pltpu.VMEM)
    done, last, scale = pl.pallas_call(
        functools.partial(kernel, times, chans, width),
        out_shape=(
            jax.ShapeDtypeStruct((batch - 1, length, channels), BF16),
            jax.ShapeDtypeStruct((length, channels), F32),
            jax.ShapeDtypeStruct((8, LANES), F32),
        ),
        in_specs=[anywhere] * 4,
        out_specs=(vmem, vmem, vmem),
        scratch_shapes=[
            big(F32), big(BF16), big(BF16), pltpu.VMEM((1, channels), F32),
            big(F32), big(BF16), big(BF16), pltpu.VMEM((batch - 1, length, channels), F32), big(F32), big(F32),
            tiles(2), tiles(times), tiles(2), tiles(batch), tiles(batch, chans),
            sems(2 * batch + 2), sems(2), sems(), sems(batch),
        ],
        compiler_params=pltpu.CompilerParams(
            collective_id=0, has_side_effects=True, vmem_limit_bytes=48 * 1024 * 1024
        ),
        name="two_way_scan",
    )(*[pltpu.with_memory_space_constraint(a, pltpu.HBM) for a in arrays])
    return pl.pallas_call(
        finish,
        out_shape=jax.ShapeDtypeStruct(shape, BF16),
        in_specs=[vmem, vmem, vmem],
        out_specs=anywhere,
        scratch_shapes=[pltpu.VMEM((length, channels), BF16), sems(length // BLOCK + 1)],
        compiler_params=pltpu.CompilerParams(vmem_limit_bytes=8 * 1024 * 1024),
        name="finish",
    )(done, last, scale)


def solution(mesh):
    spec = P("ens", "time", "chan")
    return jax.shard_map(
        functools.partial(on_device, mesh.shape["time"], mesh.shape["chan"]),
        mesh=mesh,
        in_specs=(spec, spec, spec, P(("ens", "chan"))),
        out_specs=spec,
        check_vma=False,
    )
```

```python
import functools
import math

import jax
import jax.numpy as jnp
from jax import lax
from jax.experimental import pallas as pl
from jax.experimental.pallas import tpu as pltpu
from jax.sharding import PartitionSpec as P

F32, BF16 = jnp.float32, jnp.bfloat16
BLOCK = 256
CHUNK = 32
LANES = 128


def dot(a, b):
    return lax.dot_general(a, b, (((1,), (0,)), ((), ())), preferred_element_type=F32)


def peers_by_distance(count, width):
    rows = count // width
    away = lambda s, n: min(s, n - s)
    shifts = [(r, c) for r in range(rows) for c in range(width) if r or c]
    return sorted(shifts, key=lambda s: -(away(s[0], rows) + away(s[1], width)))


class Both:
    def __init__(self, first, last):
        self.parts = first, last

    def of(self, at):
        first, last = self.parts
        return (last, at[1:]) if at[0] == first.shape[0] else (first, at)

    def __getitem__(self, at):
        ref, at = self.of(at)
        return ref[at]

    def __setitem__(self, at, value):
        ref, at = self.of(at)
        ref[at] = value


def spreader(scale):
    iota = lambda d, shape: lax.broadcasted_iota(jnp.int32, shape, d)
    square = (2 * LANES, 2 * LANES)
    ones = jnp.where((iota(0, square) % 32 < 16) == (iota(1, square) < LANES), 1.0, 0.0).astype(BF16)
    lane = iota(1, (BLOCK // 2, LANES))
    ahead = lane % 16 + lane // 32 * 16 - iota(0, (BLOCK // 2, LANES)) // 8
    high = scale.astype(BF16).astype(F32)
    tile = lambda a: jnp.concatenate([a] * (BLOCK // 16), axis=0)
    parts = tile(high), tile(scale - high)

    def block(k):
        mine = ahead == k * 16
        both = dot(jnp.concatenate([jnp.where(mine, a, 0.0).astype(BF16) for a in parts], axis=1), ones)
        return [jnp.concatenate([half, half], axis=1) for half in (both[:, :LANES], both[:, LANES:])]

    return block


def finish(done, last, scale, out_hbm, result, sem):
    before, length, channels = done.shape
    copies = [pltpu.make_async_copy(done, out_hbm.at[pl.ds(0, before)], sem.at[0])]
    copies[0].start()
    spread_over = spreader(scale[...])
    for k in range(length // BLOCK):
        for h, spread in enumerate(spread_over(k)):
            at = pl.ds(k * BLOCK + h * BLOCK // 2, BLOCK // 2)
            result[at, :] = (last[at, :] * spread).astype(BF16)
        at = pl.ds(k * BLOCK, BLOCK)
        copies.append(pltpu.make_async_copy(result.at[at, :], out_hbm.at[before, at, :], sem.at[k + 1]))
        copies[-1].start()
    for copy in copies:
        copy.wait()


def kernel(
    times, chans, width,
    decay_hbm, drive_hbm, gate_hbm, gain_hbm, done, last, last_scale,
    decay, drive, gate, gain_ref, cum, up, down, first, into, back,
    note, notes, entry, power, powers,
    in_sem, send_sem, time_recv, chan_recv,
):
    batch, length, channels = decay.shape
    blocks, halves = length // BLOCK, channels // LANES
    each = [(b, k) for b in range(batch) for k in range(blocks)]
    rows_of = lambda k: pl.ds(k * BLOCK, BLOCK)
    chunks_of = lambda k: [pl.ds(k * BLOCK + r, CHUNK) for r in range(0, BLOCK, CHUNK)]
    fold = lambda a: jnp.sum(a.reshape(CHUNK // 8, 8, a.shape[1]), axis=0)
    total = lambda a: jnp.sum(a, axis=0, keepdims=True)
    base = Both(first, last)
    to_power = math.log2(math.e) / (length * times)

    with jax.named_scope("start"):
        fetches = {}
        for b in range(batch):
            fetches["decay", b] = pltpu.make_async_copy(decay_hbm.at[b], decay.at[b], in_sem.at[2 * b])
            fetches["drive", b] = pltpu.make_async_copy(drive_hbm.at[b], drive.at[b], in_sem.at[2 * b + 1])
        fetches["gate"] = pltpu.make_async_copy(gate_hbm, gate, in_sem.at[2 * batch])
        fetches["gain"] = pltpu.make_async_copy(gain_hbm, gain_ref, in_sem.at[2 * batch + 1])
        for fetch in fetches.values():
            fetch.start()

    t_me, c_me = lax.axis_index("time"), lax.axis_index("chan")
    with jax.named_scope("greet"):
        tall = times // width
        shift = lambda at, by, count: jnp.where(at + by >= count, at + by - count, at + by)
        rows = [shift(t_me // width, r, tall) * width for r in range(tall)]
        columns = [shift(t_me % width, c, width) for c in range(width)]
        t_peers = [rows[r] + columns[c] for r, c in peers_by_distance(times, width)]
        c_peers = [shift(c_me, s, chans) for s in reversed(range(1, chans))]
        barrier = pltpu.get_barrier_semaphore()
        for peer in t_peers:
            pl.semaphore_signal(barrier, 1, device_id={"time": peer})
        for peer in c_peers:
            pl.semaphore_signal(barrier, 1, device_id={"chan": peer})

    iota = lambda d: lax.broadcasted_iota(jnp.int32, (BLOCK, BLOCK), d)
    lower = jnp.where(iota(0) >= iota(1), 1.0, 0.0).astype(BF16)
    upper = jnp.where(iota(0) <= iota(1), 1.0, 0.0).astype(BF16)

    shrink, gain_up, gain_down = {}, {}, {}

    def add_up(b, k):
        whole = plain = rising = falling = jnp.zeros((8, channels), F32)
        for at in chunks_of(k):
            logs, step = cum[b, at, :], decay[b, at, :]
            push = drive[b, at, :].astype(F32)
            u = push * (jnp.exp2(logs * to_power) - 1.0)
            v = push * (jnp.exp2((step - logs) * to_power) - 1.0)
            up[b, at, :] = u.astype(BF16)
            down[b, at, :] = v.astype(BF16)
            whole, plain = whole + fold(step), plain + fold(push)
            rising, falling = rising + fold(u), falling + fold(v)
        shrink[b, k] = jnp.exp2(total(whole) * -to_power)
        gain_up[b, k] = total(plain + rising)
        gain_down[b, k] = total(plain + falling)

    with jax.named_scope("sums"):
        for b in range(batch):
            fetches["decay", b].wait()
            fetches["drive", b].wait()
            for k in range(blocks + 1):
                if k < blocks:
                    cum[b, rows_of(k), :] = dot(lower, decay[b, rows_of(k), :].astype(BF16))
                if k > 0:
                    add_up(b, k - 1)

    with jax.named_scope("summary"):
        for b in range(batch):
            kept = shrink[b, 0]
            ahead = shrink[b, 0] * gain_up[b, 0]
            for k in range(1, blocks):
                kept = kept * shrink[b, k]
                ahead = shrink[b, k] * (ahead + gain_up[b, k])
            behind = gain_down[b, blocks - 1]
            for k in reversed(range(blocks - 1)):
                behind = shrink[b, k] * behind + gain_down[b, k]
            for h in range(halves):
                lanes = slice(h * LANES, (h + 1) * LANES)
                r = b * halves + h
                for way, state in ((0, ahead), (1, behind)):
                    note[way, r : r + 1, :] = kept[:, lanes]
                    note[way, 4 + r : 5 + r, :] = state[:, lanes]

    with jax.named_scope("meet"):
        pl.semaphore_wait(barrier, len(t_peers) + len(c_peers))

    with jax.named_scope("send"):
        instead = t_peers[0]
        ordered = [jnp.where(t_me == 0, instead, 0)]
        ordered += [jnp.where(peer == 0, instead, peer) for peer in t_peers[1:]]
        for peer in ordered:
            pltpu.make_async_remote_copy(
                src_ref=note.at[jnp.where(peer > t_me, 0, 1)],
                dst_ref=notes.at[t_me],
                send_sem=send_sem.at[0],
                recv_sem=time_recv,
                device_id={"time": peer},
            ).start()
        notes[t_me] = note[0]

    with jax.named_scope("inner"):
        fetches["gate"].wait()
        for n in range(len(each) + 1):
            if n < len(each):
                b, k = each[n]
                push = drive[b, rows_of(k), :]
                base[b, rows_of(k), :] = dot(lower, push) + dot(lower, up[b, rows_of(k), :])
                into[b, rows_of(k), :] = dot(upper, push) + dot(upper, down[b, rows_of(k), :])
            if n > 0:
                b, k = each[n - 1]
                for at in chunks_of(k):
                    logs = cum[b, at, :]
                    g = gate[b, at, :].astype(F32)
                    g = g * ((length * times) ** -0.5) / (1.0 + jnp.exp(-g))
                    p = g * jnp.exp2(logs * -to_power)
                    q = g * jnp.exp2((logs - decay[b, at, :]) * to_power)
                    base[b, at, :] = p * base[b, at, :] + q * into[b, at, :]
                    into[b, at, :] = p
                    back[b, at, :] = q

    def all_of(ref, count, sem):
        return pltpu.make_async_copy(ref.at[pl.ds(0, count)], ref.at[pl.ds(0, count)], sem)

    with jax.named_scope("receive"):
        all_of(notes, times - 1, time_recv).wait()

    with jax.named_scope("fold"):
        ahead = behind = jnp.zeros((8, LANES), F32)
        for t in range(times):
            one = notes[t]
            ahead = jnp.where(t < t_me, ahead * pltpu.roll(one, 4, 0) + one, ahead)
            one = notes[times - 1 - t]
            behind = jnp.where(times - 1 - t > t_me, behind * pltpu.roll(one, 4, 0) + one, behind)
        entry[0] = ahead
        entry[1] = behind

    with jax.named_scope("powers"):
        for b in range(batch):
            row_of = lambda way: jnp.concatenate(
                [entry[way, 4 + halves * b + h : 5 + halves * b + h, :] for h in range(halves)], axis=1
            )
            entering = {0: row_of(0)}
            for k in range(blocks - 1):
                entering[k + 1] = shrink[b, k] * (entering[k] + gain_up[b, k])
            leaving = {blocks - 1: shrink[b, blocks - 1] * row_of(1)}
            for k in reversed(range(blocks - 1)):
                leaving[k] = shrink[b, k] * (leaving[k + 1] + gain_down[b, k + 1])
            for k in range(blocks):
                for r, at in enumerate(chunks_of(k)):
                    y = base[b, at, :] + into[b, at, :] * entering[k] + back[b, at, :] * leaving[k]
                    base[b, at, :] = y
                    y = y * y
                    y = jnp.sum(y[:, :LANES] + y[:, LANES:], axis=1, keepdims=True)
                    for g in range(CHUNK // 8):
                        q = (k * BLOCK + r * CHUNK) // 8 + g
                        power[b, :, q : q + 1] = y[8 * g : 8 * g + 8]
            for peer in c_peers:
                pltpu.make_async_remote_copy(
                    src_ref=power.at[b],
                    dst_ref=powers.at[b, c_me],
                    send_sem=send_sem.at[1],
                    recv_sem=chan_recv.at[b],
                    device_id={"chan": peer},
                ).start()

    with jax.named_scope("gain"):
        fetches["gain"].wait()
        gain = gain_ref[...]
        for b, k in each:
            for at in chunks_of(k):
                base[b, at, :] = base[b, at, :] * gain

    with jax.named_scope("finish"):
        for b in range(batch):
            all_of(powers.at[b], chans - 1, chan_recv.at[b]).wait()
            powers[b, c_me] = power[b]
            squares = powers[b, 0]
            for c in range(1, chans):
                squares = squares + powers[b, c]
            scale = lax.rsqrt(squares * (1.0 / (channels * chans)) + 1e-06)
            if b < batch - 1:
                spread_over = spreader(scale)
                for k in range(blocks):
                    for h, spread in enumerate(spread_over(k)):
                        at = pl.ds(k * BLOCK + h * BLOCK // 2, BLOCK // 2)
                        done[b, at, :] = (base[b, at, :] * spread).astype(BF16)
            else:
                last_scale[...] = scale

    with jax.named_scope("drain"):
        all_of(notes, times - 1, send_sem.at[0]).wait()
        all_of(notes, batch * (chans - 1), send_sem.at[1]).wait()


def on_device(times, chans, decay_rate, drive_in, gate_in, norm_gain):
    shape = decay_rate.shape
    batch, length, channels = shape
    arrays = decay_rate, drive_in, gate_in, norm_gain.reshape(1, channels)
    width = 4 if times % 4 == 0 else 1
    big = lambda dtype: pltpu.VMEM(shape, dtype)
    tiles = lambda *lead: pltpu.VMEM((*lead, 8, LANES), F32)
    sems = lambda *dims: pltpu.SemaphoreType.DMA(dims)
    anywhere = pl.BlockSpec(memory_space=pltpu.HBM)
    vmem = pl.BlockSpec(memory_space=pltpu.VMEM)
    done, last, scale = pl.pallas_call(
        functools.partial(kernel, times, chans, width),
        out_shape=(
            jax.ShapeDtypeStruct((batch - 1, length, channels), BF16),
            jax.ShapeDtypeStruct((length, channels), F32),
            jax.ShapeDtypeStruct((8, LANES), F32),
        ),
        in_specs=[anywhere] * 4,
        out_specs=(vmem, vmem, vmem),
        scratch_shapes=[
            big(F32), big(BF16), big(BF16), pltpu.VMEM((1, channels), F32),
            big(F32), big(BF16), big(BF16), pltpu.VMEM((batch - 1, length, channels), F32), big(F32), big(F32),
            tiles(2), tiles(times), tiles(2), tiles(batch), tiles(batch, chans),
            sems(2 * batch + 2), sems(2), sems(), sems(batch),
        ],
        compiler_params=pltpu.CompilerParams(
            collective_id=0, has_side_effects=True, vmem_limit_bytes=48 * 1024 * 1024
        ),
        name="two_way_scan",
    )(*[pltpu.with_memory_space_constraint(a, pltpu.HBM) for a in arrays])
    return pl.pallas_call(
        finish,
        out_shape=jax.ShapeDtypeStruct(shape, BF16),
        in_specs=[vmem, vmem, vmem],
        out_specs=anywhere,
        scratch_shapes=[pltpu.VMEM((length, channels), BF16), sems(length // BLOCK + 1)],
        compiler_params=pltpu.CompilerParams(vmem_limit_bytes=8 * 1024 * 1024),
        name="finish",
    )(done, last, scale)


def solution(mesh):
    spec = P("ens", "time", "chan")
    return jax.shard_map(
        functools.partial(on_device, mesh.shape["time"], mesh.shape["chan"]),
        mesh=mesh,
        in_specs=(spec, spec, spec, P(("ens", "chan"))),
        out_specs=spec,
        check_vma=False,
    )
```

```python
import functools
import math

import jax
import jax.numpy as jnp
from jax import lax
from jax.experimental import pallas as pl
from jax.experimental.pallas import tpu as pltpu
from jax.sharding import PartitionSpec as P

F32, BF16 = jnp.float32, jnp.bfloat16
BLOCK = 256
CHUNK = 32
LANES = 128


def dot(a, b):
    return lax.dot_general(a, b, (((1,), (0,)), ((), ())), preferred_element_type=F32)


def peers_by_distance(count, width):
    rows = count // width
    away = lambda s, n: min(s, n - s)
    shifts = [(r, c) for r in range(rows) for c in range(width) if r or c]
    return sorted(shifts, key=lambda s: -(away(s[0], rows) + away(s[1], width)))


class Both:
    def __init__(self, first, last):
        self.parts = first, last

    def of(self, at):
        first, last = self.parts
        return (last, at[1:]) if at[0] == first.shape[0] else (first, at)

    def __getitem__(self, at):
        ref, at = self.of(at)
        return ref[at]

    def __setitem__(self, at, value):
        ref, at = self.of(at)
        ref[at] = value


def spreader(scale):
    def half(first):
        lanes = range(first, first + BLOCK // 16)
        rows = [jnp.broadcast_to(scale[:, q : q + 1], scale.shape) for q in lanes]
        both = jnp.concatenate(rows, axis=0)
        return jnp.concatenate([both, both], axis=1)

    return lambda k: [half((2 * k + h) * BLOCK // 16) for h in range(2)]


def finish(done, last, scale, out_hbm, result, sem):
    before, length, channels = done.shape
    copies = [pltpu.make_async_copy(done, out_hbm.at[pl.ds(0, before)], sem.at[0])]
    copies[0].start()
    spread_over = spreader(scale[...])
    for k in range(length // BLOCK):
        for h, spread in enumerate(spread_over(k)):
            at = pl.ds(k * BLOCK + h * BLOCK // 2, BLOCK // 2)
            result[at, :] = (last[at, :] * spread).astype(BF16)
        at = pl.ds(k * BLOCK, BLOCK)
        copies.append(pltpu.make_async_copy(result.at[at, :], out_hbm.at[before, at, :], sem.at[k + 1]))
        copies[-1].start()
    for copy in copies:
        copy.wait()


def kernel(
    times, chans, width,
    decay_hbm, drive_hbm, gate_hbm, gain_hbm, done, last, last_scale,
    decay, drive, gate, gain_ref, cum, up, down, first, into, back,
    note, notes, entry, power, powers,
    in_sem, send_sem, time_recv, chan_recv,
):
    batch, length, channels = decay.shape
    blocks, halves = length // BLOCK, channels // LANES
    each = [(b, k) for b in range(batch) for k in range(blocks)]
    rows_of = lambda k: pl.ds(k * BLOCK, BLOCK)
    chunks_of = lambda k: [pl.ds(k * BLOCK + r, CHUNK) for r in range(0, BLOCK, CHUNK)]
    fold = lambda a: jnp.sum(a.reshape(CHUNK // 8, 8, a.shape[1]), axis=0)
    total = lambda a: jnp.sum(a, axis=0, keepdims=True)
    base = Both(first, last)
    to_power = math.log2(math.e) / (length * times)

    with jax.named_scope("start"):
        fetches = {}
        for b in range(batch):
            fetches["decay", b] = pltpu.make_async_copy(decay_hbm.at[b], decay.at[b], in_sem.at[2 * b])
            fetches["drive", b] = pltpu.make_async_copy(drive_hbm.at[b], drive.at[b], in_sem.at[2 * b + 1])
        fetches["gate"] = pltpu.make_async_copy(gate_hbm, gate, in_sem.at[2 * batch])
        fetches["gain"] = pltpu.make_async_copy(gain_hbm, gain_ref, in_sem.at[2 * batch + 1])
        for fetch in fetches.values():
            fetch.start()

    t_me, c_me = lax.axis_index("time"), lax.axis_index("chan")
    with jax.named_scope("greet"):
        tall = times // width
        shift = lambda at, by, count: jnp.where(at + by >= count, at + by - count, at + by)
        rows = [shift(t_me // width, r, tall) * width for r in range(tall)]
        columns = [shift(t_me % width, c, width) for c in range(width)]
        t_peers = [rows[r] + columns[c] for r, c in peers_by_distance(times, width)]
        c_peers = [shift(c_me, s, chans) for s in reversed(range(1, chans))]
        barrier = pltpu.get_barrier_semaphore()
        for peer in t_peers:
            pl.semaphore_signal(barrier, 1, device_id={"time": peer})
        for peer in c_peers:
            pl.semaphore_signal(barrier, 1, device_id={"chan": peer})

    iota = lambda d: lax.broadcasted_iota(jnp.int32, (BLOCK, BLOCK), d)
    lower = jnp.where(iota(0) >= iota(1), 1.0, 0.0).astype(BF16)
    upper = jnp.where(iota(0) <= iota(1), 1.0, 0.0).astype(BF16)

    shrink, gain_up, gain_down = {}, {}, {}

    def add_up(b, k):
        whole = plain = rising = falling = jnp.zeros((8, channels), F32)
        for at in chunks_of(k):
            logs, step = cum[b, at, :], decay[b, at, :]
            push = drive[b, at, :].astype(F32)
            u = push * (jnp.exp2(logs * to_power) - 1.0)
            v = push * (jnp.exp2((step - logs) * to_power) - 1.0)
            up[b, at, :] = u.astype(BF16)
            down[b, at, :] = v.astype(BF16)
            whole, plain = whole + fold(step), plain + fold(push)
            rising, falling = rising + fold(u), falling + fold(v)
        shrink[b, k] = jnp.exp2(total(whole) * -to_power)
        gain_up[b, k] = total(plain + rising)
        gain_down[b, k] = total(plain + falling)

    with jax.named_scope("sums"):
        for b in range(batch):
            fetches["decay", b].wait()
            fetches["drive", b].wait()
            for k in range(blocks + 1):
                if k < blocks:
                    cum[b, rows_of(k), :] = dot(lower, decay[b, rows_of(k), :].astype(BF16))
                if k > 0:
                    add_up(b, k - 1)

    with jax.named_scope("summary"):
        for b in range(batch):
            kept = shrink[b, 0]
            ahead = shrink[b, 0] * gain_up[b, 0]
            for k in range(1, blocks):
                kept = kept * shrink[b, k]
                ahead = shrink[b, k] * (ahead + gain_up[b, k])
            behind = gain_down[b, blocks - 1]
            for k in reversed(range(blocks - 1)):
                behind = shrink[b, k] * behind + gain_down[b, k]
            for h in range(halves):
                lanes = slice(h * LANES, (h + 1) * LANES)
                r = b * halves + h
                for way, state in ((0, ahead), (1, behind)):
                    note[way, r : r + 1, :] = kept[:, lanes]
                    note[way, 4 + r : 5 + r, :] = state[:, lanes]

    with jax.named_scope("meet"):
        pl.semaphore_wait(barrier, len(t_peers) + len(c_peers))

    with jax.named_scope("send"):
        instead = t_peers[0]
        ordered = [jnp.where(t_me == 0, instead, 0)]
        ordered += [jnp.where(peer == 0, instead, peer) for peer in t_peers[1:]]
        for peer in ordered:
            pltpu.make_async_remote_copy(
                src_ref=note.at[jnp.where(peer > t_me, 0, 1)],
                dst_ref=notes.at[t_me],
                send_sem=send_sem.at[0],
                recv_sem=time_recv,
                device_id={"time": peer},
            ).start()
        notes[t_me] = note[0]

    with jax.named_scope("inner"):
        fetches["gate"].wait()
        for n in range(len(each) + 1):
            if n < len(each):
                b, k = each[n]
                push = drive[b, rows_of(k), :]
                base[b, rows_of(k), :] = dot(lower, push) + dot(lower, up[b, rows_of(k), :])
                into[b, rows_of(k), :] = dot(upper, push) + dot(upper, down[b, rows_of(k), :])
            if n > 0:
                b, k = each[n - 1]
                for at in chunks_of(k):
                    logs = cum[b, at, :]
                    g = gate[b, at, :].astype(F32)
                    g = g * ((length * times) ** -0.5) / (1.0 + jnp.exp(-g))
                    p = g * jnp.exp2(logs * -to_power)
                    q = g * jnp.exp2((logs - decay[b, at, :]) * to_power)
                    base[b, at, :] = p * base[b, at, :] + q * into[b, at, :]
                    into[b, at, :] = p
                    back[b, at, :] = q

    def all_of(ref, count, sem):
        return pltpu.make_async_copy(ref.at[pl.ds(0, count)], ref.at[pl.ds(0, count)], sem)

    with jax.named_scope("receive"):
        all_of(notes, times - 1, time_recv).wait()

    with jax.named_scope("fold"):
        ahead = behind = jnp.zeros((8, LANES), F32)
        for t in range(times):
            one = notes[t]
            ahead = jnp.where(t < t_me, ahead * pltpu.roll(one, 4, 0) + one, ahead)
            one = notes[times - 1 - t]
            behind = jnp.where(times - 1 - t > t_me, behind * pltpu.roll(one, 4, 0) + one, behind)
        entry[0] = ahead
        entry[1] = behind

    with jax.named_scope("powers"):
        for b in range(batch):
            row_of = lambda way: jnp.concatenate(
                [entry[way, 4 + halves * b + h : 5 + halves * b + h, :] for h in range(halves)], axis=1
            )
            entering = {0: row_of(0)}
            for k in range(blocks - 1):
                entering[k + 1] = shrink[b, k] * (entering[k] + gain_up[b, k])
            leaving = {blocks - 1: shrink[b, blocks - 1] * row_of(1)}
            for k in reversed(range(blocks - 1)):
                leaving[k] = shrink[b, k] * (leaving[k + 1] + gain_down[b, k + 1])
            for k in range(blocks):
                for r, at in enumerate(chunks_of(k)):
                    y = base[b, at, :] + into[b, at, :] * entering[k] + back[b, at, :] * leaving[k]
                    base[b, at, :] = y
                    y = y * y
                    y = jnp.sum(y[:, :LANES] + y[:, LANES:], axis=1, keepdims=True)
                    for g in range(CHUNK // 8):
                        q = (k * BLOCK + r * CHUNK) // 8 + g
                        power[b, :, q : q + 1] = y[8 * g : 8 * g + 8]
            for peer in c_peers:
                pltpu.make_async_remote_copy(
                    src_ref=power.at[b],
                    dst_ref=powers.at[b, c_me],
                    send_sem=send_sem.at[1],
                    recv_sem=chan_recv.at[b],
                    device_id={"chan": peer},
                ).start()

    with jax.named_scope("gain"):
        fetches["gain"].wait()
        gain = gain_ref[...]
        for b, k in each:
            for at in chunks_of(k):
                base[b, at, :] = base[b, at, :] * gain

    with jax.named_scope("finish"):
        for b in range(batch):
            all_of(powers.at[b], chans - 1, chan_recv.at[b]).wait()
            powers[b, c_me] = power[b]
            squares = powers[b, 0]
            for c in range(1, chans):
                squares = squares + powers[b, c]
            scale = lax.rsqrt(squares * (1.0 / (channels * chans)) + 1e-06)
            if b < batch - 1:
                spread_over = spreader(scale)
                for k in range(blocks):
                    for h, spread in enumerate(spread_over(k)):
                        at = pl.ds(k * BLOCK + h * BLOCK // 2, BLOCK // 2)
                        done[b, at, :] = (base[b, at, :] * spread).astype(BF16)
            else:
                last_scale[...] = scale

    with jax.named_scope("drain"):
        all_of(notes, times - 1, send_sem.at[0]).wait()
        all_of(notes, batch * (chans - 1), send_sem.at[1]).wait()


def on_device(times, chans, decay_rate, drive_in, gate_in, norm_gain):
    shape = decay_rate.shape
    batch, length, channels = shape
    arrays = decay_rate, drive_in, gate_in, norm_gain.reshape(1, channels)
    width = 4 if times % 4 == 0 else 1
    big = lambda dtype: pltpu.VMEM(shape, dtype)
    tiles = lambda *lead: pltpu.VMEM((*lead, 8, LANES), F32)
    sems = lambda *dims: pltpu.SemaphoreType.DMA(dims)
    anywhere = pl.BlockSpec(memory_space=pltpu.HBM)
    vmem = pl.BlockSpec(memory_space=pltpu.VMEM)
    done, last, scale = pl.pallas_call(
        functools.partial(kernel, times, chans, width),
        out_shape=(
            jax.ShapeDtypeStruct((batch - 1, length, channels), BF16),
            jax.ShapeDtypeStruct((length, channels), F32),
            jax.ShapeDtypeStruct((8, LANES), F32),
        ),
        in_specs=[anywhere] * 4,
        out_specs=(vmem, vmem, vmem),
        scratch_shapes=[
            big(F32), big(BF16), big(BF16), pltpu.VMEM((1, channels), F32),
            big(F32), big(BF16), big(BF16), pltpu.VMEM((batch - 1, length, channels), F32), big(F32), big(F32),
            tiles(2), tiles(times), tiles(2), tiles(batch), tiles(batch, chans),
            sems(2 * batch + 2), sems(2), sems(), sems(batch),
        ],
        compiler_params=pltpu.CompilerParams(
            collective_id=0, has_side_effects=True, vmem_limit_bytes=48 * 1024 * 1024
        ),
        name="two_way_scan",
    )(*[pltpu.with_memory_space_constraint(a, pltpu.HBM) for a in arrays])
    return pl.pallas_call(
        finish,
        out_shape=jax.ShapeDtypeStruct(shape, BF16),
        in_specs=[vmem, vmem, vmem],
        out_specs=anywhere,
        scratch_shapes=[pltpu.VMEM((length, channels), BF16), sems(length // BLOCK + 1)],
        compiler_params=pltpu.CompilerParams(vmem_limit_bytes=8 * 1024 * 1024),
        name="finish",
    )(done, last, scale)


def solution(mesh):
    spec = P("ens", "time", "chan")
    return jax.shard_map(
        functools.partial(on_device, mesh.shape["time"], mesh.shape["chan"]),
        mesh=mesh,
        in_specs=(spec, spec, spec, P(("ens", "chan"))),
        out_specs=spec,
        check_vma=False,
    )
```

```python
import functools
import math

import jax
import jax.numpy as jnp
from jax import lax
from jax.experimental import pallas as pl
from jax.experimental.pallas import tpu as pltpu
from jax.sharding import PartitionSpec as P

F32, BF16 = jnp.float32, jnp.bfloat16
BLOCK = 256
CHUNK = 32
LANES = 128


def dot(a, b):
    return lax.dot_general(a, b, (((1,), (0,)), ((), ())), preferred_element_type=F32)


def peers_by_distance(count, width):
    rows = count // width
    away = lambda s, n: min(s, n - s)
    shifts = [(r, c) for r in range(rows) for c in range(width) if r or c]
    return sorted(shifts, key=lambda s: -(away(s[0], rows) + away(s[1], width)))


class Both:
    def __init__(self, first, last):
        self.parts = first, last

    def of(self, at):
        first, last = self.parts
        return (last, at[1:]) if at[0] == first.shape[0] else (first, at)

    def __getitem__(self, at):
        ref, at = self.of(at)
        return ref[at]

    def __setitem__(self, at, value):
        ref, at = self.of(at)
        ref[at] = value


def spreader(scale):
    def half(first):
        lanes = range(first, first + BLOCK // 16)
        rows = [jnp.broadcast_to(scale[:, q : q + 1], scale.shape) for q in lanes]
        both = jnp.concatenate(rows, axis=0)
        return jnp.concatenate([both, both], axis=1)

    return lambda k: [half((2 * k + h) * BLOCK // 16) for h in range(2)]


def finish(done, last, scale, out_hbm, result, sem):
    before, length, channels = done.shape
    pltpu.make_async_copy(done, out_hbm.at[pl.ds(0, before)], sem).start()
    spread_over = spreader(scale[...])
    for k in range(length // BLOCK):
        for h, spread in enumerate(spread_over(k)):
            at = pl.ds(k * BLOCK + h * BLOCK // 2, BLOCK // 2)
            result[at, :] = (last[at, :] * spread).astype(BF16)
        at = pl.ds(k * BLOCK, BLOCK)
        pltpu.make_async_copy(result.at[at, :], out_hbm.at[before, at, :], sem).start()
    pltpu.make_async_copy(out_hbm, out_hbm, sem).wait()


def kernel(
    times, chans, width,
    decay_hbm, drive_hbm, gate_hbm, gain_hbm, done, last, last_scale,
    decay, drive, gate, gain_ref, cum, up, down, first, into, back,
    note, notes, entry, power, powers,
    in_sem, send_sem, time_recv, chan_recv,
):
    batch, length, channels = decay.shape
    blocks, halves = length // BLOCK, channels // LANES
    each = [(b, k) for b in range(batch) for k in range(blocks)]
    rows_of = lambda k: pl.ds(k * BLOCK, BLOCK)
    chunks_of = lambda k: [pl.ds(k * BLOCK + r, CHUNK) for r in range(0, BLOCK, CHUNK)]
    fold = lambda a: jnp.sum(a.reshape(CHUNK // 8, 8, a.shape[1]), axis=0)
    total = lambda a: jnp.sum(a, axis=0, keepdims=True)
    base = Both(first, last)
    to_power = math.log2(math.e) / (length * times)

    with jax.named_scope("start"):
        fetches = {}
        for b in range(batch):
            fetches["decay", b] = pltpu.make_async_copy(decay_hbm.at[b], decay.at[b], in_sem.at[2 * b])
            fetches["drive", b] = pltpu.make_async_copy(drive_hbm.at[b], drive.at[b], in_sem.at[2 * b + 1])
        fetches["gate"] = pltpu.make_async_copy(gate_hbm, gate, in_sem.at[2 * batch])
        fetches["gain"] = pltpu.make_async_copy(gain_hbm, gain_ref, in_sem.at[2 * batch + 1])
        for fetch in fetches.values():
            fetch.start()

    t_me, c_me = lax.axis_index("time"), lax.axis_index("chan")
    with jax.named_scope("greet"):
        tall = times // width
        shift = lambda at, by, count: jnp.where(at + by >= count, at + by - count, at + by)
        rows = [shift(t_me // width, r, tall) * width for r in range(tall)]
        columns = [shift(t_me % width, c, width) for c in range(width)]
        t_peers = [rows[r] + columns[c] for r, c in peers_by_distance(times, width)]
        c_peers = [shift(c_me, s, chans) for s in reversed(range(1, chans))]
        barrier = pltpu.get_barrier_semaphore()
        for peer in t_peers:
            pl.semaphore_signal(barrier, 1, device_id={"time": peer})
        for peer in c_peers:
            pl.semaphore_signal(barrier, 1, device_id={"chan": peer})

    iota = lambda d: lax.broadcasted_iota(jnp.int32, (BLOCK, BLOCK), d)
    lower = jnp.where(iota(0) >= iota(1), 1.0, 0.0).astype(BF16)
    upper = jnp.where(iota(0) <= iota(1), 1.0, 0.0).astype(BF16)

    shrink, gain_up, gain_down = {}, {}, {}

    def add_up(b, k):
        whole = plain = rising = falling = jnp.zeros((8, channels), F32)
        for at in chunks_of(k):
            logs, step = cum[b, at, :], decay[b, at, :]
            push = drive[b, at, :].astype(F32)
            u = push * (jnp.exp2(logs * to_power) - 1.0)
            v = push * (jnp.exp2((step - logs) * to_power) - 1.0)
            up[b, at, :] = u.astype(BF16)
            down[b, at, :] = v.astype(BF16)
            whole, plain = whole + fold(step), plain + fold(push)
            rising, falling = rising + fold(u), falling + fold(v)
        shrink[b, k] = jnp.exp2(total(whole) * -to_power)
        gain_up[b, k] = total(plain + rising)
        gain_down[b, k] = total(plain + falling)

    with jax.named_scope("sums"):
        for b in range(batch):
            fetches["decay", b].wait()
            fetches["drive", b].wait()
            for k in range(blocks + 1):
                if k < blocks:
                    cum[b, rows_of(k), :] = dot(lower, decay[b, rows_of(k), :].astype(BF16))
                if k > 0:
                    add_up(b, k - 1)

    with jax.named_scope("summary"):
        for b in range(batch):
            kept = shrink[b, 0]
            ahead = shrink[b, 0] * gain_up[b, 0]
            for k in range(1, blocks):
                kept = kept * shrink[b, k]
                ahead = shrink[b, k] * (ahead + gain_up[b, k])
            behind = gain_down[b, blocks - 1]
            for k in reversed(range(blocks - 1)):
                behind = shrink[b, k] * behind + gain_down[b, k]
            for h in range(halves):
                lanes = slice(h * LANES, (h + 1) * LANES)
                r = b * halves + h
                for way, state in ((0, ahead), (1, behind)):
                    note[way, r : r + 1, :] = kept[:, lanes]
                    note[way, 4 + r : 5 + r, :] = state[:, lanes]

    with jax.named_scope("meet"):
        pl.semaphore_wait(barrier, len(t_peers) + len(c_peers))

    with jax.named_scope("send"):
        instead = t_peers[0]
        ordered = [jnp.where(t_me == 0, instead, 0)]
        ordered += [jnp.where(peer == 0, instead, peer) for peer in t_peers[1:]]
        for peer in ordered:
            pltpu.make_async_remote_copy(
                src_ref=note.at[jnp.where(peer > t_me, 0, 1)],
                dst_ref=notes.at[t_me],
                send_sem=send_sem.at[0],
                recv_sem=time_recv,
                device_id={"time": peer},
            ).start()
        notes[t_me] = note[0]

    with jax.named_scope("inner"):
        fetches["gate"].wait()
        for n in range(len(each) + 1):
            if n < len(each):
                b, k = each[n]
                push = drive[b, rows_of(k), :]
                base[b, rows_of(k), :] = dot(lower, push) + dot(lower, up[b, rows_of(k), :])
                into[b, rows_of(k), :] = dot(upper, push) + dot(upper, down[b, rows_of(k), :])
            if n > 0:
                b, k = each[n - 1]
                for at in chunks_of(k):
                    logs = cum[b, at, :]
                    g = gate[b, at, :].astype(F32)
                    g = g * ((length * times) ** -0.5) / (1.0 + jnp.exp(-g))
                    p = g * jnp.exp2(logs * -to_power)
                    q = g * jnp.exp2((logs - decay[b, at, :]) * to_power)
                    base[b, at, :] = p * base[b, at, :] + q * into[b, at, :]
                    into[b, at, :] = p
                    back[b, at, :] = q

    def all_of(ref, count, sem):
        return pltpu.make_async_copy(ref.at[pl.ds(0, count)], ref.at[pl.ds(0, count)], sem)

    with jax.named_scope("receive"):
        all_of(notes, times - 1, time_recv).wait()

    with jax.named_scope("fold"):
        ahead = behind = jnp.zeros((8, LANES), F32)
        for t in range(times):
            one = notes[t]
            ahead = jnp.where(t < t_me, ahead * pltpu.roll(one, 4, 0) + one, ahead)
            one = notes[times - 1 - t]
            behind = jnp.where(times - 1 - t > t_me, behind * pltpu.roll(one, 4, 0) + one, behind)
        entry[0] = ahead
        entry[1] = behind

    with jax.named_scope("powers"):
        for b in range(batch):
            row_of = lambda way: jnp.concatenate(
                [entry[way, 4 + halves * b + h : 5 + halves * b + h, :] for h in range(halves)], axis=1
            )
            entering = {0: row_of(0)}
            for k in range(blocks - 1):
                entering[k + 1] = shrink[b, k] * (entering[k] + gain_up[b, k])
            leaving = {blocks - 1: shrink[b, blocks - 1] * row_of(1)}
            for k in reversed(range(blocks - 1)):
                leaving[k] = shrink[b, k] * (leaving[k + 1] + gain_down[b, k + 1])
            for k in range(blocks):
                for r, at in enumerate(chunks_of(k)):
                    y = base[b, at, :] + into[b, at, :] * entering[k] + back[b, at, :] * leaving[k]
                    base[b, at, :] = y
                    y = y * y
                    y = jnp.sum(y[:, :LANES] + y[:, LANES:], axis=1, keepdims=True)
                    for g in range(CHUNK // 8):
                        q = (k * BLOCK + r * CHUNK) // 8 + g
                        power[b, :, q : q + 1] = y[8 * g : 8 * g + 8]
            for peer in c_peers:
                pltpu.make_async_remote_copy(
                    src_ref=power.at[b],
                    dst_ref=powers.at[b, c_me],
                    send_sem=send_sem.at[1],
                    recv_sem=chan_recv.at[b],
                    device_id={"chan": peer},
                ).start()

    with jax.named_scope("gain"):
        fetches["gain"].wait()
        gain = gain_ref[...]
        for b, k in each:
            for at in chunks_of(k):
                base[b, at, :] = base[b, at, :] * gain

    with jax.named_scope("finish"):
        for b in range(batch):
            all_of(powers.at[b], chans - 1, chan_recv.at[b]).wait()
            powers[b, c_me] = power[b]
            squares = powers[b, 0]
            for c in range(1, chans):
                squares = squares + powers[b, c]
            scale = lax.rsqrt(squares * (1.0 / (channels * chans)) + 1e-06)
            if b < batch - 1:
                spread_over = spreader(scale)
                for k in range(blocks):
                    for h, spread in enumerate(spread_over(k)):
                        at = pl.ds(k * BLOCK + h * BLOCK // 2, BLOCK // 2)
                        done[b, at, :] = (base[b, at, :] * spread).astype(BF16)
            else:
                last_scale[...] = scale

    with jax.named_scope("drain"):
        all_of(notes, times - 1, send_sem.at[0]).wait()
        all_of(notes, batch * (chans - 1), send_sem.at[1]).wait()


def on_device(times, chans, decay_rate, drive_in, gate_in, norm_gain):
    shape = decay_rate.shape
    batch, length, channels = shape
    arrays = decay_rate, drive_in, gate_in, norm_gain.reshape(1, channels)
    width = 4 if times % 4 == 0 else 1
    big = lambda dtype: pltpu.VMEM(shape, dtype)
    tiles = lambda *lead: pltpu.VMEM((*lead, 8, LANES), F32)
    sems = lambda *dims: pltpu.SemaphoreType.DMA(dims)
    anywhere = pl.BlockSpec(memory_space=pltpu.HBM)
    vmem = pl.BlockSpec(memory_space=pltpu.VMEM)
    done, last, scale = pl.pallas_call(
        functools.partial(kernel, times, chans, width),
        out_shape=(
            jax.ShapeDtypeStruct((batch - 1, length, channels), BF16),
            jax.ShapeDtypeStruct((length, channels), F32),
            jax.ShapeDtypeStruct((8, LANES), F32),
        ),
        in_specs=[anywhere] * 4,
        out_specs=(vmem, vmem, vmem),
        scratch_shapes=[
            big(F32), big(BF16), big(BF16), pltpu.VMEM((1, channels), F32),
            big(F32), big(BF16), big(BF16), pltpu.VMEM((batch - 1, length, channels), F32), big(F32), big(F32),
            tiles(2), tiles(times), tiles(2), tiles(batch), tiles(batch, chans),
            sems(2 * batch + 2), sems(2), sems(), sems(batch),
        ],
        compiler_params=pltpu.CompilerParams(
            collective_id=0, has_side_effects=True, vmem_limit_bytes=48 * 1024 * 1024
        ),
        name="two_way_scan",
    )(*[pltpu.with_memory_space_constraint(a, pltpu.HBM) for a in arrays])
    return pl.pallas_call(
        finish,
        out_shape=jax.ShapeDtypeStruct(shape, BF16),
        in_specs=[vmem, vmem, vmem],
        out_specs=anywhere,
        scratch_shapes=[pltpu.VMEM((length, channels), BF16), sems()],
        compiler_params=pltpu.CompilerParams(vmem_limit_bytes=8 * 1024 * 1024),
        name="finish",
    )(done, last, scale)


def solution(mesh):
    spec = P("ens", "time", "chan")
    return jax.shard_map(
        functools.partial(on_device, mesh.shape["time"], mesh.shape["chan"]),
        mesh=mesh,
        in_specs=(spec, spec, spec, P(("ens", "chan"))),
        out_specs=spec,
        check_vma=False,
    )
```

```python
import functools
import math

import jax
import jax.numpy as jnp
from jax import lax
from jax.experimental import pallas as pl
from jax.experimental.pallas import tpu as pltpu
from jax.sharding import PartitionSpec as P

F32, BF16 = jnp.float32, jnp.bfloat16
BLOCK = 256
CHUNK = 32
LANES = 128


def dot(a, b):
    return lax.dot_general(a, b, (((1,), (0,)), ((), ())), preferred_element_type=F32)


def peers_by_distance(count, width):
    rows = count // width
    away = lambda s, n: min(s, n - s)
    shifts = [(r, c) for r in range(rows) for c in range(width) if r or c]
    return sorted(shifts, key=lambda s: -(away(s[0], rows) + away(s[1], width)))


class Both:
    def __init__(self, first, last):
        self.parts = first, last

    def of(self, at):
        first, last = self.parts
        return (last, at[1:]) if at[0] == first.shape[0] else (first, at)

    def __getitem__(self, at):
        ref, at = self.of(at)
        return ref[at]

    def __setitem__(self, at, value):
        ref, at = self.of(at)
        ref[at] = value


def spreader(scale):
    def half(first):
        lanes = range(first, first + BLOCK // 16)
        rows = [jnp.broadcast_to(scale[:, q : q + 1], scale.shape) for q in lanes]
        both = jnp.concatenate(rows, axis=0)
        return jnp.concatenate([both, both], axis=1)

    return lambda k: [half((2 * k + h) * BLOCK // 16) for h in range(2)]


def finish(done, last, scale, out_hbm, result, sem):
    before, length, channels = done.shape
    pltpu.make_async_copy(done, out_hbm.at[pl.ds(0, before)], sem).start()
    spread_over = spreader(scale[...])
    for k in range(length // BLOCK):
        for h, spread in enumerate(spread_over(k)):
            at = pl.ds(k * BLOCK + h * BLOCK // 2, BLOCK // 2)
            result[at, :] = (last[at, :] * spread).astype(BF16)
        at = pl.ds(k * BLOCK, BLOCK)
        pltpu.make_async_copy(result.at[at, :], out_hbm.at[before, at, :], sem).start()
    pltpu.make_async_copy(out_hbm, out_hbm, sem).wait()


def kernel(
    times, chans, width,
    decay_hbm, drive_hbm, gate_hbm, gain_hbm, done, last, last_scale,
    decay, drive, gate, gain_ref, cum, up, down, first, into, back,
    note, notes, entry, power, powers,
    in_sem, send_sem, time_recv, chan_recv,
):
    batch, length, channels = decay.shape
    blocks, halves = length // BLOCK, channels // LANES
    each = [(b, k) for b in range(batch) for k in range(blocks)]
    rows_of = lambda k: pl.ds(k * BLOCK, BLOCK)
    chunks_of = lambda k: [pl.ds(k * BLOCK + r, CHUNK) for r in range(0, BLOCK, CHUNK)]
    fold = lambda a: jnp.sum(a.reshape(CHUNK // 8, 8, a.shape[1]), axis=0)
    total = lambda a: jnp.sum(a, axis=0, keepdims=True)
    base = Both(first, last)
    to_power = math.log2(math.e) / (length * times)

    with jax.named_scope("start"):
        fetches = {}
        for b in range(batch):
            fetches["decay", b] = pltpu.make_async_copy(decay_hbm.at[b], decay.at[b], in_sem.at[b])
            fetches["drive", b] = pltpu.make_async_copy(drive_hbm.at[b], drive.at[b], in_sem.at[b])
        fetches["gate"] = pltpu.make_async_copy(gate_hbm, gate, in_sem.at[batch])
        fetches["gain"] = pltpu.make_async_copy(gain_hbm, gain_ref, in_sem.at[batch + 1])
        for fetch in fetches.values():
            fetch.start()

    t_me, c_me = lax.axis_index("time"), lax.axis_index("chan")
    with jax.named_scope("greet"):
        tall = times // width
        shift = lambda at, by, count: jnp.where(at + by >= count, at + by - count, at + by)
        rows = [shift(t_me // width, r, tall) * width for r in range(tall)]
        columns = [shift(t_me % width, c, width) for c in range(width)]
        t_peers = [rows[r] + columns[c] for r, c in peers_by_distance(times, width)]
        c_peers = [shift(c_me, s, chans) for s in reversed(range(1, chans))]
        barrier = pltpu.get_barrier_semaphore()
        for peer in t_peers:
            pl.semaphore_signal(barrier, 1, device_id={"time": peer})
        for peer in c_peers:
            pl.semaphore_signal(barrier, 1, device_id={"chan": peer})

    iota = lambda d: lax.broadcasted_iota(jnp.int32, (BLOCK, BLOCK), d)
    lower = jnp.where(iota(0) >= iota(1), 1.0, 0.0).astype(BF16)
    upper = jnp.where(iota(0) <= iota(1), 1.0, 0.0).astype(BF16)

    shrink, gain_up, gain_down = {}, {}, {}

    def add_up(b, k):
        whole = plain = rising = falling = jnp.zeros((8, channels), F32)
        for at in chunks_of(k):
            logs, step = cum[b, at, :], decay[b, at, :]
            push = drive[b, at, :].astype(F32)
            u = push * (jnp.exp2(logs * to_power) - 1.0)
            v = push * (jnp.exp2((step - logs) * to_power) - 1.0)
            up[b, at, :] = u.astype(BF16)
            down[b, at, :] = v.astype(BF16)
            whole, plain = whole + fold(step), plain + fold(push)
            rising, falling = rising + fold(u), falling + fold(v)
        shrink[b, k] = jnp.exp2(total(whole) * -to_power)
        gain_up[b, k] = total(plain + rising)
        gain_down[b, k] = total(plain + falling)

    with jax.named_scope("sums"):
        for b in range(batch):
            both = decay.at[pl.ds(0, 2), pl.ds(0, length * 3 // 4), :]
            pltpu.make_async_copy(both, both, in_sem.at[b]).wait()
            for k in range(blocks + 1):
                if k < blocks:
                    cum[b, rows_of(k), :] = dot(lower, decay[b, rows_of(k), :].astype(BF16))
                if k > 0:
                    add_up(b, k - 1)

    with jax.named_scope("summary"):
        for b in range(batch):
            kept = shrink[b, 0]
            ahead = shrink[b, 0] * gain_up[b, 0]
            for k in range(1, blocks):
                kept = kept * shrink[b, k]
                ahead = shrink[b, k] * (ahead + gain_up[b, k])
            behind = gain_down[b, blocks - 1]
            for k in reversed(range(blocks - 1)):
                behind = shrink[b, k] * behind + gain_down[b, k]
            for h in range(halves):
                lanes = slice(h * LANES, (h + 1) * LANES)
                r = b * halves + h
                for way, state in ((0, ahead), (1, behind)):
                    note[way, r : r + 1, :] = kept[:, lanes]
                    note[way, 4 + r : 5 + r, :] = state[:, lanes]

    with jax.named_scope("meet"):
        pl.semaphore_wait(barrier, len(t_peers) + len(c_peers))

    with jax.named_scope("send"):
        instead = t_peers[0]
        ordered = [jnp.where(t_me == 0, instead, 0)]
        ordered += [jnp.where(peer == 0, instead, peer) for peer in t_peers[1:]]
        for peer in ordered:
            pltpu.make_async_remote_copy(
                src_ref=note.at[jnp.where(peer > t_me, 0, 1)],
                dst_ref=notes.at[t_me],
                send_sem=send_sem.at[0],
                recv_sem=time_recv,
                device_id={"time": peer},
            ).start()
        notes[t_me] = note[0]

    with jax.named_scope("inner"):
        fetches["gate"].wait()
        for n in range(len(each) + 1):
            if n < len(each):
                b, k = each[n]
                push = drive[b, rows_of(k), :]
                base[b, rows_of(k), :] = dot(lower, push) + dot(lower, up[b, rows_of(k), :])
                into[b, rows_of(k), :] = dot(upper, push) + dot(upper, down[b, rows_of(k), :])
            if n > 0:
                b, k = each[n - 1]
                for at in chunks_of(k):
                    logs = cum[b, at, :]
                    g = gate[b, at, :].astype(F32)
                    g = g * ((length * times) ** -0.5) / (1.0 + jnp.exp(-g))
                    p = g * jnp.exp2(logs * -to_power)
                    q = g * jnp.exp2((logs - decay[b, at, :]) * to_power)
                    base[b, at, :] = p * base[b, at, :] + q * into[b, at, :]
                    into[b, at, :] = p
                    back[b, at, :] = q

    def all_of(ref, count, sem):
        return pltpu.make_async_copy(ref.at[pl.ds(0, count)], ref.at[pl.ds(0, count)], sem)

    with jax.named_scope("receive"):
        all_of(notes, times - 1, time_recv).wait()

    with jax.named_scope("fold"):
        ahead = behind = jnp.zeros((8, LANES), F32)
        for t in range(times):
            one = notes[t]
            ahead = jnp.where(t < t_me, ahead * pltpu.roll(one, 4, 0) + one, ahead)
            one = notes[times - 1 - t]
            behind = jnp.where(times - 1 - t > t_me, behind * pltpu.roll(one, 4, 0) + one, behind)
        entry[0] = ahead
        entry[1] = behind

    with jax.named_scope("powers"):
        for b in range(batch):
            row_of = lambda way: jnp.concatenate(
                [entry[way, 4 + halves * b + h : 5 + halves * b + h, :] for h in range(halves)], axis=1
            )
            entering = {0: row_of(0)}
            for k in range(blocks - 1):
                entering[k + 1] = shrink[b, k] * (entering[k] + gain_up[b, k])
            leaving = {blocks - 1: shrink[b, blocks - 1] * row_of(1)}
            for k in reversed(range(blocks - 1)):
                leaving[k] = shrink[b, k] * (leaving[k + 1] + gain_down[b, k + 1])
            for k in range(blocks):
                for r, at in enumerate(chunks_of(k)):
                    y = base[b, at, :] + into[b, at, :] * entering[k] + back[b, at, :] * leaving[k]
                    base[b, at, :] = y
                    y = y * y
                    y = jnp.sum(y[:, :LANES] + y[:, LANES:], axis=1, keepdims=True)
                    for g in range(CHUNK // 8):
                        q = (k * BLOCK + r * CHUNK) // 8 + g
                        power[b, :, q : q + 1] = y[8 * g : 8 * g + 8]
            for peer in c_peers:
                pltpu.make_async_remote_copy(
                    src_ref=power.at[b],
                    dst_ref=powers.at[b, c_me],
                    send_sem=send_sem.at[1],
                    recv_sem=chan_recv.at[b],
                    device_id={"chan": peer},
                ).start()

    with jax.named_scope("gain"):
        fetches["gain"].wait()
        gain = gain_ref[...]
        for b, k in each:
            for at in chunks_of(k):
                base[b, at, :] = base[b, at, :] * gain

    with jax.named_scope("finish"):
        for b in range(batch):
            all_of(powers.at[b], chans - 1, chan_recv.at[b]).wait()
            powers[b, c_me] = power[b]
            squares = powers[b, 0]
            for c in range(1, chans):
                squares = squares + powers[b, c]
            scale = lax.rsqrt(squares * (1.0 / (channels * chans)) + 1e-06)
            if b < batch - 1:
                spread_over = spreader(scale)
                for k in range(blocks):
                    for h, spread in enumerate(spread_over(k)):
                        at = pl.ds(k * BLOCK + h * BLOCK // 2, BLOCK // 2)
                        done[b, at, :] = (base[b, at, :] * spread).astype(BF16)
            else:
                last_scale[...] = scale

    with jax.named_scope("drain"):
        all_of(notes, times - 1, send_sem.at[0]).wait()
        all_of(notes, batch * (chans - 1), send_sem.at[1]).wait()


def on_device(times, chans, decay_rate, drive_in, gate_in, norm_gain):
    shape = decay_rate.shape
    batch, length, channels = shape
    arrays = decay_rate, drive_in, gate_in, norm_gain.reshape(1, channels)
    width = 4 if times % 4 == 0 else 1
    big = lambda dtype: pltpu.VMEM(shape, dtype)
    tiles = lambda *lead: pltpu.VMEM((*lead, 8, LANES), F32)
    sems = lambda *dims: pltpu.SemaphoreType.DMA(dims)
    anywhere = pl.BlockSpec(memory_space=pltpu.HBM)
    vmem = pl.BlockSpec(memory_space=pltpu.VMEM)
    done, last, scale = pl.pallas_call(
        functools.partial(kernel, times, chans, width),
        out_shape=(
            jax.ShapeDtypeStruct((batch - 1, length, channels), BF16),
            jax.ShapeDtypeStruct((length, channels), F32),
            jax.ShapeDtypeStruct((8, LANES), F32),
        ),
        in_specs=[anywhere] * 4,
        out_specs=(vmem, vmem, vmem),
        scratch_shapes=[
            big(F32), big(BF16), big(BF16), pltpu.VMEM((1, channels), F32),
            big(F32), big(BF16), big(BF16), pltpu.VMEM((batch - 1, length, channels), F32), big(F32), big(F32),
            tiles(2), tiles(times), tiles(2), tiles(batch), tiles(batch, chans),
            sems(batch + 2), sems(2), sems(), sems(batch),
        ],
        compiler_params=pltpu.CompilerParams(
            collective_id=0, has_side_effects=True, vmem_limit_bytes=48 * 1024 * 1024
        ),
        name="two_way_scan",
    )(*[pltpu.with_memory_space_constraint(a, pltpu.HBM) for a in arrays])
    return pl.pallas_call(
        finish,
        out_shape=jax.ShapeDtypeStruct(shape, BF16),
        in_specs=[vmem, vmem, vmem],
        out_specs=anywhere,
        scratch_shapes=[pltpu.VMEM((length, channels), BF16), sems()],
        compiler_params=pltpu.CompilerParams(vmem_limit_bytes=8 * 1024 * 1024),
        name="finish",
    )(done, last, scale)


def solution(mesh):
    spec = P("ens", "time", "chan")
    return jax.shard_map(
        functools.partial(on_device, mesh.shape["time"], mesh.shape["chan"]),
        mesh=mesh,
        in_specs=(spec, spec, spec, P(("ens", "chan"))),
        out_specs=spec,
        check_vma=False,
    )
```

```python
import functools
import math

import jax
import jax.numpy as jnp
from jax import lax
from jax.experimental import pallas as pl
from jax.experimental.pallas import tpu as pltpu
from jax.sharding import PartitionSpec as P

F32, BF16 = jnp.float32, jnp.bfloat16
BLOCK = 256
CHUNK = 32
LANES = 128


def dot(a, b):
    return lax.dot_general(a, b, (((1,), (0,)), ((), ())), preferred_element_type=F32)


def peers_by_distance(count, width):
    rows = count // width
    away = lambda s, n: min(s, n - s)
    shifts = [(r, c) for r in range(rows) for c in range(width) if r or c]
    return sorted(shifts, key=lambda s: -(away(s[0], rows) + away(s[1], width)))


class Both:
    def __init__(self, first, last):
        self.parts = first, last

    def of(self, at):
        first, last = self.parts
        return (last, at[1:]) if at[0] == first.shape[0] else (first, at)

    def __getitem__(self, at):
        ref, at = self.of(at)
        return ref[at]

    def __setitem__(self, at, value):
        ref, at = self.of(at)
        ref[at] = value


def spreader(scale):
    def half(first):
        lanes = range(first, first + BLOCK // 16)
        rows = [jnp.broadcast_to(scale[:, q : q + 1], scale.shape) for q in lanes]
        both = jnp.concatenate(rows, axis=0)
        return jnp.concatenate([both, both], axis=1)

    return lambda k: [half((2 * k + h) * BLOCK // 16) for h in range(2)]


def finish(done, last, scale, out_hbm, result, sem):
    before, length, channels = done.shape
    pltpu.make_async_copy(done, out_hbm.at[pl.ds(0, before)], sem).start()
    spread_over = spreader(scale[...])
    for k in range(length // BLOCK):
        for h, spread in enumerate(spread_over(k)):
            at = pl.ds(k * BLOCK + h * BLOCK // 2, BLOCK // 2)
            result[at, :] = (last[at, :] * spread).astype(BF16)
        at = pl.ds(k * BLOCK, BLOCK)
        pltpu.make_async_copy(result.at[at, :], out_hbm.at[before, at, :], sem).start()
    pltpu.make_async_copy(out_hbm, out_hbm, sem).wait()


def kernel(
    times, chans, width,
    decay_hbm, drive_hbm, gate_hbm, gain_hbm, done, last, last_scale,
    decay, drive, gate, gain_ref, cum, up, down, first, into, back,
    note, notes, entry, power, powers,
    in_sem, send_sem, time_recv, chan_recv,
):
    batch, length, channels = decay.shape
    blocks, halves = length // BLOCK, channels // LANES
    each = [(b, k) for b in range(batch) for k in range(blocks)]
    rows_of = lambda k: pl.ds(k * BLOCK, BLOCK)
    chunks_of = lambda k: [pl.ds(k * BLOCK + r, CHUNK) for r in range(0, BLOCK, CHUNK)]
    fold = lambda a: jnp.sum(a.reshape(CHUNK // 8, 8, a.shape[1]), axis=0)
    total = lambda a: jnp.sum(a, axis=0, keepdims=True)
    base = Both(first, last)
    to_power = math.log2(math.e) / (length * times)

    with jax.named_scope("start"):
        fetches = {}
        for b in range(batch):
            fetches["decay", b] = pltpu.make_async_copy(decay_hbm.at[b], decay.at[b], in_sem.at[b])
            fetches["drive", b] = pltpu.make_async_copy(drive_hbm.at[b], drive.at[b], in_sem.at[b])
        fetches["gate"] = pltpu.make_async_copy(gate_hbm, gate, in_sem.at[batch])
        fetches["gain"] = pltpu.make_async_copy(gain_hbm, gain_ref, in_sem.at[batch + 1])
        for fetch in fetches.values():
            fetch.start()

    t_me, c_me = lax.axis_index("time"), lax.axis_index("chan")
    with jax.named_scope("greet"):
        tall = times // width
        shift = lambda at, by, count: jnp.where(at + by >= count, at + by - count, at + by)
        rows = [shift(t_me // width, r, tall) * width for r in range(tall)]
        columns = [shift(t_me % width, c, width) for c in range(width)]
        t_peers = [rows[r] + columns[c] for r, c in peers_by_distance(times, width)]
        c_peers = [shift(c_me, s, chans) for s in reversed(range(1, chans))]
        barrier = pltpu.get_barrier_semaphore()
        for peer in t_peers:
            pl.semaphore_signal(barrier, 1, device_id={"time": peer})
        for peer in c_peers:
            pl.semaphore_signal(barrier, 1, device_id={"chan": peer})

    iota = lambda d: lax.broadcasted_iota(jnp.int32, (BLOCK, BLOCK), d)
    lower = jnp.where(iota(0) >= iota(1), 1.0, 0.0).astype(BF16)
    upper = jnp.where(iota(0) <= iota(1), 1.0, 0.0).astype(BF16)

    shrink, gain_up, gain_down = {}, {}, {}

    def add_up(b, k):
        whole = plain = rising = falling = jnp.zeros((8, channels), F32)
        for at in chunks_of(k):
            logs, step = cum[b, at, :], decay[b, at, :]
            push = drive[b, at, :].astype(F32)
            u = push * (jnp.exp2(logs * to_power) - 1.0)
            v = push * (jnp.exp2((step - logs) * to_power) - 1.0)
            up[b, at, :] = u.astype(BF16)
            down[b, at, :] = v.astype(BF16)
            whole, plain = whole + fold(step), plain + fold(push)
            rising, falling = rising + fold(u), falling + fold(v)
        shrink[b, k] = jnp.exp2(total(whole) * -to_power)
        gain_up[b, k] = total(plain + rising)
        gain_down[b, k] = total(plain + falling)

    with jax.named_scope("sums"):
        for b in range(batch):
            both = decay.at[pl.ds(0, 2), pl.ds(0, length * 3 // 4), :]
            pltpu.make_async_copy(both, both, in_sem.at[b]).wait()
            for k in range(blocks + 1):
                if k < blocks:
                    cum[b, rows_of(k), :] = dot(lower, decay[b, rows_of(k), :].astype(BF16))
                if k > 0:
                    add_up(b, k - 1)

    with jax.named_scope("summary"):
        for b in range(batch):
            kept = shrink[b, 0]
            ahead = shrink[b, 0] * gain_up[b, 0]
            for k in range(1, blocks):
                kept = kept * shrink[b, k]
                ahead = shrink[b, k] * (ahead + gain_up[b, k])
            behind = gain_down[b, blocks - 1]
            for k in reversed(range(blocks - 1)):
                behind = shrink[b, k] * behind + gain_down[b, k]
            for h in range(halves):
                lanes = slice(h * LANES, (h + 1) * LANES)
                r = b * halves + h
                for way, state in ((0, ahead), (1, behind)):
                    note[way, r : r + 1, :] = kept[:, lanes]
                    note[way, 4 + r : 5 + r, :] = state[:, lanes]

    with jax.named_scope("meet"):
        pl.semaphore_wait(barrier, len(t_peers) + len(c_peers))

    with jax.named_scope("send"):
        instead = t_peers[0]
        ordered = [jnp.where(t_me == 0, instead, 0)]
        ordered += [jnp.where(peer == 0, instead, peer) for peer in t_peers[1:]]
        for peer in ordered:
            pltpu.make_async_remote_copy(
                src_ref=note.at[jnp.where(peer > t_me, 0, 1)],
                dst_ref=notes.at[t_me],
                send_sem=send_sem.at[0],
                recv_sem=time_recv,
                device_id={"time": peer},
            ).start()
        notes[t_me] = note[0]

    with jax.named_scope("inner"):
        fetches["gate"].wait()
        for n in range(len(each) + 1):
            if n < len(each):
                b, k = each[n]
                push = drive[b, rows_of(k), :]
                base[b, rows_of(k), :] = dot(lower, push) + dot(lower, up[b, rows_of(k), :])
                into[b, rows_of(k), :] = dot(upper, push) + dot(upper, down[b, rows_of(k), :])
            if n > 0:
                b, k = each[n - 1]
                for at in chunks_of(k):
                    logs = cum[b, at, :]
                    g = gate[b, at, :].astype(F32)
                    g = g * ((length * times) ** -0.5) / (1.0 + jnp.exp(-g))
                    p = g * jnp.exp2(logs * -to_power)
                    q = g * jnp.exp2((logs - decay[b, at, :]) * to_power)
                    base[b, at, :] = p * base[b, at, :] + q * into[b, at, :]
                    into[b, at, :] = p
                    back[b, at, :] = q

    def all_of(ref, count, sem):
        return pltpu.make_async_copy(ref.at[pl.ds(0, count)], ref.at[pl.ds(0, count)], sem)

    with jax.named_scope("receive"):
        all_of(notes, times - 1, time_recv).wait()

    with jax.named_scope("fold"):
        nothing = jnp.where(lax.broadcasted_iota(jnp.int32, (8, LANES), 0) < 4, 1.0, 0.0)

        def chain(ts, counts):
            kept = state = None
            for t in ts:
                one = jnp.where(counts(t), notes[t], nothing)
                keep = pltpu.roll(one, 4, 0)
                kept, state = (keep, one) if state is None else (kept * keep, state * keep + one)
            return kept, state

        def both(ts, counts):
            _, state = chain(ts[: len(ts) // 2], counts)
            kept, more = chain(ts[len(ts) // 2 :], counts)
            return state * kept + more

        ahead = both(list(range(times)), lambda t: t < t_me)
        behind = both(list(reversed(range(times))), lambda t: t > t_me)
        entry[0] = ahead
        entry[1] = behind

    with jax.named_scope("powers"):
        for b in range(batch):
            row_of = lambda way: jnp.concatenate(
                [entry[way, 4 + halves * b + h : 5 + halves * b + h, :] for h in range(halves)], axis=1
            )
            entering = {0: row_of(0)}
            for k in range(blocks - 1):
                entering[k + 1] = shrink[b, k] * (entering[k] + gain_up[b, k])
            leaving = {blocks - 1: shrink[b, blocks - 1] * row_of(1)}
            for k in reversed(range(blocks - 1)):
                leaving[k] = shrink[b, k] * (leaving[k + 1] + gain_down[b, k + 1])
            for k in range(blocks):
                for r, at in enumerate(chunks_of(k)):
                    y = base[b, at, :] + into[b, at, :] * entering[k] + back[b, at, :] * leaving[k]
                    base[b, at, :] = y
                    y = y * y
                    y = jnp.sum(y[:, :LANES] + y[:, LANES:], axis=1, keepdims=True)
                    for g in range(CHUNK // 8):
                        q = (k * BLOCK + r * CHUNK) // 8 + g
                        power[b, :, q : q + 1] = y[8 * g : 8 * g + 8]
            for peer in c_peers:
                pltpu.make_async_remote_copy(
                    src_ref=power.at[b],
                    dst_ref=powers.at[b, c_me],
                    send_sem=send_sem.at[1],
                    recv_sem=chan_recv.at[b],
                    device_id={"chan": peer},
                ).start()

    with jax.named_scope("gain"):
        fetches["gain"].wait()
        gain = gain_ref[...]
        for b, k in each:
            for at in chunks_of(k):
                base[b, at, :] = base[b, at, :] * gain

    with jax.named_scope("finish"):
        for b in range(batch):
            all_of(powers.at[b], chans - 1, chan_recv.at[b]).wait()
            powers[b, c_me] = power[b]
            squares = powers[b, 0]
            for c in range(1, chans):
                squares = squares + powers[b, c]
            scale = lax.rsqrt(squares * (1.0 / (channels * chans)) + 1e-06)
            if b < batch - 1:
                spread_over = spreader(scale)
                for k in range(blocks):
                    for h, spread in enumerate(spread_over(k)):
                        at = pl.ds(k * BLOCK + h * BLOCK // 2, BLOCK // 2)
                        done[b, at, :] = (base[b, at, :] * spread).astype(BF16)
            else:
                last_scale[...] = scale

    with jax.named_scope("drain"):
        all_of(notes, times - 1, send_sem.at[0]).wait()
        all_of(notes, batch * (chans - 1), send_sem.at[1]).wait()


def on_device(times, chans, decay_rate, drive_in, gate_in, norm_gain):
    shape = decay_rate.shape
    batch, length, channels = shape
    arrays = decay_rate, drive_in, gate_in, norm_gain.reshape(1, channels)
    width = 4 if times % 4 == 0 else 1
    big = lambda dtype: pltpu.VMEM(shape, dtype)
    tiles = lambda *lead: pltpu.VMEM((*lead, 8, LANES), F32)
    sems = lambda *dims: pltpu.SemaphoreType.DMA(dims)
    anywhere = pl.BlockSpec(memory_space=pltpu.HBM)
    vmem = pl.BlockSpec(memory_space=pltpu.VMEM)
    done, last, scale = pl.pallas_call(
        functools.partial(kernel, times, chans, width),
        out_shape=(
            jax.ShapeDtypeStruct((batch - 1, length, channels), BF16),
            jax.ShapeDtypeStruct((length, channels), F32),
            jax.ShapeDtypeStruct((8, LANES), F32),
        ),
        in_specs=[anywhere] * 4,
        out_specs=(vmem, vmem, vmem),
        scratch_shapes=[
            big(F32), big(BF16), big(BF16), pltpu.VMEM((1, channels), F32),
            big(F32), big(BF16), big(BF16), pltpu.VMEM((batch - 1, length, channels), F32), big(F32), big(F32),
            tiles(2), tiles(times), tiles(2), tiles(batch), tiles(batch, chans),
            sems(batch + 2), sems(2), sems(), sems(batch),
        ],
        compiler_params=pltpu.CompilerParams(
            collective_id=0, has_side_effects=True, vmem_limit_bytes=48 * 1024 * 1024
        ),
        name="two_way_scan",
    )(*[pltpu.with_memory_space_constraint(a, pltpu.HBM) for a in arrays])
    return pl.pallas_call(
        finish,
        out_shape=jax.ShapeDtypeStruct(shape, BF16),
        in_specs=[vmem, vmem, vmem],
        out_specs=anywhere,
        scratch_shapes=[pltpu.VMEM((length, channels), BF16), sems()],
        compiler_params=pltpu.CompilerParams(vmem_limit_bytes=8 * 1024 * 1024),
        name="finish",
    )(done, last, scale)


def solution(mesh):
    spec = P("ens", "time", "chan")
    return jax.shard_map(
        functools.partial(on_device, mesh.shape["time"], mesh.shape["chan"]),
        mesh=mesh,
        in_specs=(spec, spec, spec, P(("ens", "chan"))),
        out_specs=spec,
        check_vma=False,
    )
```
